512 devices in a mesh: row: 16 (over z), col: 32 (over y, x, core).
Axes of the slice: x: 4, y: 4, z: 16, core: 2. Of those that a mesh axis runs over, the one named last changes fastest.
Arguments:
- momentum: float32 [8192, 26624], P('row', 'col'), may hold values from -6 to 6
- gradient: bfloat16 [8192, 26624], P('row', 'col'), may hold values from -150 to 150
- q_basis: bfloat16 [26624, 512], P('col', 'row'), may hold values from -0.0390625 to 0.0390625
Outputs:
- momentum_next: float32 [8192, 26624], P('row', 'col')
- p_basis: float32 [8192, 512], P(('row', 'col'))
- q_next: float32 [26624, 512], P('col', 'row')
The draws below stay inside these ranges and needn't reach their ends.
All inputs are finite; a program needn't handle non-finite values.
Results may differ from the reference program's by a relative error of at most 0.0065.
Values may be sent and summed in bfloat16 or wider, within the bound.
A program may use at most 64 MiB of HBM per device.

```python
import math
import jax
import jax.numpy as jnp
from jax import lax

ROWS = 8192
COLS = 26624
RANK = 512


def draw_gradient(key, part):
    base_key = jax.random.fold_in(key, 17)
    streams = jax.random.split(base_key, 6)
    signal_rank = RANK // 2
    row_ramp = jnp.exp(math.log(3.0) * jnp.arange(ROWS, dtype=jnp.float32) / ROWS)
    col_ramp = jnp.exp(math.log(3.0) * jnp.arange(COLS, dtype=jnp.float32) / COLS)
    values = jax.random.truncated_normal(streams[0], -4.0, 4.0, (ROWS, COLS), jnp.float32)
    row_rough = jnp.exp(jax.random.uniform(streams[1], (ROWS,), jnp.float32, 0.0, math.log(2.0)))
    col_rough = jnp.exp(jax.random.uniform(streams[2], (COLS,), jnp.float32, 0.0, math.log(2.0)))
    target = 6.0
    strengths = jnp.exp(jax.random.uniform(streams[3], (signal_rank,), jnp.float32, 0.0, math.log(4.0)))
    left_factor = jax.random.normal(streams[4], (ROWS, signal_rank), jnp.float32)
    right_factor = jax.random.normal(streams[5], (COLS, signal_rank), jnp.float32)
    weighting = target / 3.64 * strengths / jnp.sqrt(jnp.sum(strengths * strengths))
    signal = jnp.dot(left_factor * weighting[None, :], right_factor.T, precision=lax.Precision.HIGHEST)
    noise = 0.25 * values * (row_ramp * row_rough)[:, None] * (col_ramp * col_rough)[None, :]
    scaled = noise + signal * row_ramp[:, None] * col_ramp[None, :]
    return jnp.clip(scaled, -150.0, 150.0).astype(jnp.bfloat16)


def block_scale(own_key, shape, pieces, least, top_value):
    level, own = 1.0, jax.random.fold_in(own_key, 6)
    for axis_at, blocks in pieces:
        draws = jnp.exp(jax.random.uniform(jax.random.fold_in(own, axis_at), (blocks,), jnp.float32, least / len(pieces), top_value / len(pieces)))
        level = level * jnp.repeat(draws, shape[axis_at] // blocks).reshape([-1 if axis == axis_at else 1 for axis in range(len(shape))])
    return level


def centred(key, extent, scale, limit, shards=(), held_as=jnp.bfloat16):
    array = scale * jax.random.normal(key, extent, jnp.float32)
    if shards:
        array = array * block_scale(key, extent, shards, -0.22, 0.18)
    return jnp.clip(array, -limit, limit).astype(held_as)


def setup_inputs(seed: int = 0) -> dict:
    keys = jax.random.split(jax.random.key(seed), 4)
    return {
        "momentum": centred(keys[0], (ROWS, COLS), 1.0, 6.0, ((0, 16), (1, 32)), jnp.float32),
        "gradient": draw_gradient(jax.random.fold_in(keys[3], 71), 0),
        "q_basis": centred(keys[2], (COLS, RANK), COLS ** -0.5, 0.0390625, ((0, 32), (1, 16))),
    }


def reference(momentum, gradient, q_basis):
    buffer = momentum + gradient.astype(jnp.float32)
    buffer_low = buffer.astype(jnp.bfloat16)
    power = jnp.dot(buffer_low.astype(jnp.float32), q_basis.astype(jnp.float32), preferred_element_type=jnp.float32)
    gram = jnp.dot(power.T, power, precision=lax.Precision.HIGHEST)
    lower = jnp.linalg.cholesky(gram)
    p_basis = jax.scipy.linalg.solve_triangular(lower, power.T, lower=True).T
    p_low = p_basis.astype(jnp.bfloat16)
    right = jnp.dot(buffer_low.T.astype(jnp.float32), p_low.astype(jnp.float32), preferred_element_type=jnp.float32)
    sums = lax.optimization_barrier(jnp.sum(right * right, axis=0))
    q_next = right / jnp.sqrt(sums + 1e-06)
    right_low = right.astype(jnp.bfloat16)
    update = jnp.dot(p_low.astype(jnp.float32), right_low.T.astype(jnp.float32), preferred_element_type=jnp.float32)
    return (buffer - 0.1 * update, p_basis, q_next)
```

```python
import jax
import jax.numpy as jnp
from jax import lax
from jax.experimental import pallas as pl
from jax.experimental.pallas import tpu as pltpu
from jax.sharding import PartitionSpec as P

HI = lax.Precision.HIGHEST
MESH = pl.DeviceIdType.MESH
F32, BF16 = jnp.float32, jnp.bfloat16
NB = 128
DMA = pltpu.SemaphoreType.DMA
NT = (((1,), (1,)), ((), ()))
TN = (((0,), (0,)), ((), ()))


def send(src, dst, send_sem, recv_sem, **where):
    copy = pltpu.make_async_remote_copy(
        src_ref=src, dst_ref=dst, send_sem=send_sem, recv_sem=recv_sem, device_id=where, device_id_type=MESH
    )
    copy.start()
    return copy


def drain(view, sem):
    pltpu.make_async_copy(view, view, sem).wait()


def greet(z, c, nz, nc, near):
    barrier = pltpu.get_barrier_semaphore()
    if near:
        for step in (1, nz - 1):
            pl.semaphore_signal(barrier, inc=1, device_id={"row": lax.rem(z + step, nz)}, device_id_type=MESH)
    else:
        @pl.loop(1, nz)
        def _(j):
            pl.semaphore_signal(barrier, inc=1, device_id={"row": lax.rem(z + j, nz)}, device_id_type=MESH)

    @pl.loop(1, nc)
    def _(j):
        pl.semaphore_signal(barrier, inc=1, device_id={"col": lax.rem(c + j, nc)}, device_id_type=MESH)

    def met():
        pl.semaphore_wait(barrier, (2 if near else nz - 1) + nc - 1)

    return met


class Ring:
    def __init__(self, held, send_sems, recv_sems, z, nz):
        self.held, self.ss, self.rs = held, send_sems, recv_sems
        self.nz, self.half = nz, nz // 2
        self.ways = (lax.rem(z + 1, nz), lax.rem(z + nz - 1, nz))
        self.sent, self.got = [], set()

    def arrived(self, slot, chunk):
        if slot != 0 and (slot, chunk) not in self.got:
            self.got.add((slot, chunk))
            drain(self.held.at[slot, chunk], self.rs.at[slot, chunk])

    def step(self, t):
        for chunk in (0, 1):
            for way in (0, 1):
                if t == self.half and chunk != way:
                    continue
                src, dst = (t - 1, t) if way == 0 else ((self.nz - t + 1) % self.nz, self.nz - t)
                self.arrived(src, chunk)
                self.sent.append(send(
                    self.held.at[src, chunk], self.held.at[dst, chunk],
                    self.ss.at[way, t - 1, chunk], self.rs.at[dst, chunk], row=self.ways[way]))

    def slot_arrived(self, slot):
        for chunk in (0, 1):
            self.arrived(slot, chunk)

    def finish(self):
        for copy in self.sent:
            copy.wait_send()


def power_kernel(
    nz, nc, mom_ref, grad_ref, q_ref, w_ref, g_ref,
    blow, held, parts, came, shares, gpart, gcame, grow, gall,
    q_ss, q_rs, c_ss, c_rs, a_ss, a_rs, d_ss, d_rs, z_ss, z_rs, y_ss, y_rs, g_ss, g_rs, e_ss, e_rs,
):
    z, c = lax.axis_index("row"), lax.axis_index("col")
    chip, core = lax.div(c, 2), lax.rem(c, 2)
    partner = chip * 2 + 1 - core
    chips, half = nc // 2, nz // 2
    met = greet(z, c, nz, nc, False)
    blow[...] = (mom_ref[...] + grad_ref[...].astype(F32)).astype(BF16)
    rows = blow.shape[1]
    lanes = rows // 128
    wide = q_ref.shape[0]
    for chunk in (0, 1):
        held[0, chunk] = q_ref[chunk * (wide // 2):(chunk + 1) * (wide // 2), :]
    met()
    ring = Ring(held, q_ss, q_rs, z, nz)
    sides = [(t, (nz - t) % nz if t else half) for t in range(half)]

    def multiply(p):
        for slot in sides[p]:
            ring.slot_arrived(slot)
        lhs = jnp.concatenate([held[slot].reshape(wide, -1) for slot in sides[p]], axis=0)
        prod = jnp.dot(lhs, blow[...], preferred_element_type=F32)
        for side in (0, 1):
            for piece in range(chips):
                s, l = piece // lanes, piece % lanes
                parts[p, side, piece] = prod[side * wide + 8 * s:side * wide + 8 * s + 8, 128 * l:128 * l + 128]
        came[p, c] = parts[p, core, chip]

        @pl.loop(1, nc)
        def _(j):
            to = lax.rem(c + j, nc)
            send(parts.at[p, lax.rem(to, 2), lax.div(to, 2)], came.at[p, c], c_ss.at[p], c_rs.at[p], col=to)

    def add_up(p):
        drain(came.at[p, pl.ds(0, nc - 1)], c_rs.at[p])
        shares[p, core, chip] = came[p].sum(axis=0)

        @pl.loop(1, chips)
        def _(j):
            to = lax.rem(chip + j, chips) * 2 + core
            mine = shares.at[p, core, chip]
            send(mine, mine, a_ss.at[p], a_rs.at[p], col=to)

    def cross(p):
        drain(shares.at[p, core, pl.ds(0, chips - 1)], a_rs.at[p])
        view = shares.at[p, core]
        send(view, view, d_ss.at[p], d_rs.at[p], col=partner)

    order = list(range(1, half)) + [0]
    ring.step(1)
    for i in range(half + 4):
        if i + 2 <= half:
            ring.step(i + 2)
        if i < half:
            multiply(order[i])
        if 0 <= i - 2 < half:
            add_up(order[i - 2])
        if 0 <= i - 4 < half:
            cross(order[i - 4])
    for p in range(half):
        drain(shares.at[p, core], d_rs.at[p])
    for p in range(half):
        for side in (0, 1):
            at = lax.rem(z + nz - sides[p][side], nz) * wide
            for piece in range(chips):
                s, l = piece // lanes, piece % lanes
                w_ref[pl.ds(pl.multiple_of(at + 8 * s, 8), 8), 128 * l:128 * l + 128] = shares[p, side, piece]

    share = w_ref.shape[0] // nc
    mine = w_ref[pl.ds(pl.multiple_of(c * share, share), share), :]
    prod = lax.dot_general(mine, w_ref[...], NT, precision=HI, preferred_element_type=F32)
    glanes = prod.shape[1] // 128
    tall = share * glanes // nz
    for piece in range(nz):
        s, l = piece // glanes, piece % glanes
        gpart[piece] = prod[tall * s:tall * (s + 1), 128 * l:128 * l + 128]
    gcame[z] = gpart[z]

    @pl.loop(1, nz)
    def _(j):
        to = lax.rem(z + j, nz)
        send(gpart.at[to], gcame.at[z], z_ss, z_rs, row=to)

    drain(gcame.at[pl.ds(0, nz - 1)], z_rs)
    grow[z] = gcame[...].sum(axis=0)

    @pl.loop(1, nz)
    def _(j):
        to = lax.rem(z + j, nz)
        send(grow.at[z], grow.at[z], y_ss, y_rs, row=to)

    drain(grow.at[pl.ds(0, nz - 1)], y_rs)
    gall[core, chip] = grow[...]

    @pl.loop(1, chips)
    def _(j):
        to = lax.rem(chip + j, chips) * 2 + core
        mine = gall.at[core, chip]
        send(mine, mine, g_ss, g_rs, col=to)

    drain(gall.at[core, pl.ds(0, chips - 1)], g_rs)
    across = send(gall.at[core], gall.at[core], e_ss, e_rs, col=partner)
    ring.finish()
    for p in range(half):
        drain(came.at[p, pl.ds(0, nc - 1)], c_ss.at[p])
        drain(shares.at[p, core, pl.ds(0, chips - 1)], a_ss.at[p])
        drain(shares.at[p, core], d_ss.at[p])
    drain(gcame.at[pl.ds(0, nz - 1)], z_ss)
    drain(grow.at[pl.ds(0, nz - 1)], y_ss)
    drain(gall.at[core, pl.ds(0, chips - 1)], g_ss)
    across.wait()
    for other in range(nc):
        for piece in range(nz):
            s, l = piece // glanes, piece % glanes
            top = other * share + tall * s
            g_ref[top:top + tall, 128 * l:128 * l + 128] = gall[other % 2, other // 2, piece]


def power_and_gram(mom, grad, q, nz, nc):
    cols, rows = mom.shape
    wide = q.shape[0]
    rank, half, chips = wide * nz, nz // 2, nc // 2
    share = rank // nc
    tall = share * (rank // 128) // nz
    whole = pl.BlockSpec(memory_space=pltpu.VMEM)
    return pl.pallas_call(
        lambda *refs: power_kernel(nz, nc, *refs),
        out_shape=(jax.ShapeDtypeStruct((rank, rows), F32), jax.ShapeDtypeStruct((rank, rank), F32)),
        in_specs=[whole] * 3,
        out_specs=(whole, whole),
        scratch_shapes=[
            pltpu.VMEM((cols, rows), BF16),
            pltpu.VMEM((nz, 2, wide // 2, cols), BF16),
            pltpu.VMEM((half, 2, chips, 8, 128), F32),
            pltpu.VMEM((half, nc, 8, 128), F32),
            pltpu.VMEM((half, 2, chips, 8, 128), F32),
            pltpu.VMEM((nz, tall, 128), F32),
            pltpu.VMEM((nz, tall, 128), F32),
            pltpu.VMEM((nz, tall, 128), F32),
            pltpu.VMEM((2, chips, nz, tall, 128), F32),
            DMA((2, half, 2)), DMA((nz, 2)),
            DMA((half,)), DMA((half,)), DMA((half,)), DMA((half,)), DMA((half,)), DMA((half,)),
            DMA, DMA, DMA, DMA, DMA, DMA, DMA, DMA,
        ],
        compiler_params=pltpu.CompilerParams(
            collective_id=0, has_side_effects=True, vmem_limit_bytes=40 * 1024 * 1024),
        name="power_and_gram",
    )(mom, grad, q)


def sub_bcast(x, j):
    return jnp.broadcast_to(x[j:j + 1, :], x.shape)


def lane_bcast(x, j):
    return jnp.broadcast_to(x[:, j:j + 1], x.shape)


def diag_inverse(d_ref, inv_ref):
    n = NB // 8
    row = lax.broadcasted_iota(jnp.int32, (8, NB), 0)
    lane = lax.broadcasted_iota(jnp.int32, (8, NB), 1)
    for g in range(n):
        inv_ref[8 * g:8 * g + 8, :] = jnp.where(row + 8 * g == lane, 1.0, 0.0).astype(jnp.float32)
    for s in range(n):
        rd = d_ref[8 * s:8 * s + 8, :]
        ri = inv_ref[8 * s:8 * s + 8, :]
        c = [lane_bcast(rd, 8 * s + k) for k in range(8)]
        u = {}
        scale = []
        ud = []
        ui = []
        for j in range(8):
            rs = lax.rsqrt(sub_bcast(c[j], j))
            scale.append(rs)
            lj = jnp.where(row > j, c[j] * rs, 0.0)
            for k in range(j + 1, 8):
                u[j, k] = sub_bcast(c[k], j) * rs
                c[k] = c[k] - lj * u[j, k]
            ud.append(sub_bcast(rd, j) * rs)
            ui.append(sub_bcast(ri, j) * rs)
            rd = rd - lj * ud[j]
            ri = ri - lj * ui[j]
        out = ui[7]
        for j in range(7):
            out = jnp.where(row == j, ui[j], out)
        inv_ref[8 * s:8 * s + 8, :] = out
        for g in range(s + 1, n):
            rd = d_ref[8 * g:8 * g + 8, :]
            ri = inv_ref[8 * g:8 * g + 8, :]
            c = [lane_bcast(rd, 8 * s + k) for k in range(8)]
            for j in range(8):
                lj = c[j] * scale[j]
                for k in range(j + 1, 8):
                    c[k] = c[k] - lj * u[j, k]
                rd = rd - lj * ud[j]
                ri = ri - lj * ui[j]
            d_ref[8 * g:8 * g + 8, :] = rd
            inv_ref[8 * g:8 * g + 8, :] = ri


def solve_kernel(g_ref, w_ref, low_ref, p_ref, a, d, inv, pt):
    rank = w_ref.shape[0]
    rows = w_ref.shape[1]
    blocks = rank // NB
    a[:, :rank] = g_ref[...]
    a[:, rank:] = w_ref[...]

    def step(b, carry):
        at = pl.multiple_of(b * NB, NB)
        d[...] = a[pl.ds(at, NB), pl.ds(at, NB)]
        diag_inverse(d, inv)
        for bb in range(blocks):
            @pl.when(b == bb)
            def _():
                lo, hi = bb * NB, (bb + 1) * NB
                y = jnp.dot(inv[...], a[lo:hi, hi:], precision=HI, preferred_element_type=jnp.float32)
                x = y[:, rank - hi:]
                a[lo:hi, rank:] = x
                if bb < blocks - 1:
                    ut = y[:, :rank - hi].T
                    a[hi:rank, hi:] = a[hi:rank, hi:] - jnp.dot(
                        ut, y, precision=HI, preferred_element_type=jnp.float32)
        return carry

    lax.fori_loop(0, blocks, step, 0)
    full = a[:, rank:]
    low_ref[...] = full.astype(jnp.bfloat16)
    pt[...] = full.T
    share = p_ref.shape[0]
    mine = lax.axis_index("col") * share
    p_ref[...] = pt[pl.ds(pl.multiple_of(mine, share), share), :]


def solve(gram, w, share):
    rank, rows = w.shape
    whole = pl.BlockSpec(memory_space=pltpu.VMEM)
    return pl.pallas_call(
        solve_kernel,
        out_shape=(jax.ShapeDtypeStruct((rank, rows), jnp.bfloat16), jax.ShapeDtypeStruct((share, rank), jnp.float32)),
        in_specs=[whole, whole],
        out_specs=(whole, whole),
        scratch_shapes=[
            pltpu.VMEM((rank, rank + rows), jnp.float32),
            pltpu.VMEM((NB, NB), jnp.float32),
            pltpu.VMEM((NB, NB), jnp.float32),
            pltpu.VMEM((rows, rank), jnp.float32),
        ],
        compiler_params=pltpu.CompilerParams(vmem_limit_bytes=40 * 1024 * 1024),
        name="solve",
    )(gram, w)


def right_kernel(
    nz, nc, mom_ref, grad_ref, p_ref, out_ref, q_ref,
    blow, part, stage, came, cols, held, turned, sums, sums_came,
    r_ss, r_rs, q_ss, q_rs, n_ss, n_rs,
):
    z, c = lax.axis_index("row"), lax.axis_index("col")
    half = nz // 2
    met = greet(z, c, nz, nc, True)
    blow[...] = (mom_ref[...] + grad_ref[...].astype(F32)).astype(BF16)
    wide = q_ref.shape[0]
    thin = wide // 2
    prod = lax.dot_general(p_ref[...], blow[...], NT, preferred_element_type=F32)
    for block in range(nz):
        for chunk in (0, 1):
            at = block * wide + chunk * thin
            part[block, chunk] = prod[at:at + thin, :]
    met()
    ways = (lax.rem(z + nz - 1, nz), lax.rem(z + 1, nz))
    sent = []
    for s in range(half):
        for chunk in (0, 1):
            for way in (0, 1):
                first = int(chunk != way)
                if s < first:
                    continue
                far = half - s
                target = lax.rem(z + (nz - far if way == 0 else far), nz)
                value = part[target, chunk]
                if s > first:
                    drain(came.at[way, s - 1, chunk], r_rs.at[way, s - 1, chunk])
                    value = value + came[way, s - 1, chunk].astype(F32)
                stage[way, s, chunk] = value.astype(BF16)
                sent.append(send(
                    stage.at[way, s, chunk], came.at[way, s, chunk],
                    r_ss.at[way, s, chunk], r_rs.at[way, s, chunk], row=ways[way]))
    total = jnp.zeros((wide, 1), F32)
    both = []
    for chunk in (0, 1):
        value = part[z, chunk]
        for way in (0, 1):
            drain(came.at[way, half - 1, chunk], r_rs.at[way, half - 1, chunk])
            value = value + came[way, half - 1, chunk].astype(F32)
        cols[chunk] = value
        held[0, chunk] = value.astype(BF16)
    ring = Ring(held, q_ss, q_rs, z, nz)
    ring.step(1)
    value = cols[...].reshape(wide, -1)
    sums[...] = jnp.broadcast_to(jnp.sum(value * value, axis=1, keepdims=True), (wide, 128))
    sums_came[c] = sums[...]

    @pl.loop(1, nc)
    def _(j):
        send(sums, sums_came.at[c], n_ss, n_rs, col=lax.rem(c + j, nc))

    for slot in range(nz):
        at = lax.rem(z + nz - slot, nz) * wide
        turned[wide * slot:wide * (slot + 1), :] = p_ref[pl.ds(pl.multiple_of(at, wide), wide), :]
    for t in range(2, half + 1):
        ring.step(t)
        if t == half - 1:
            drain(sums_came.at[pl.ds(0, nc - 1)], n_rs)
            norms = jnp.sqrt(jnp.sum(sums_came[...], axis=0)[:, :1] + 1e-06)
            q_ref[...] = value / norms
    for slot in range(nz):
        ring.slot_arrived(slot)
    right = held[...].reshape(nz * wide, -1)
    update = lax.dot_general(right, turned[...], TN, preferred_element_type=F32)
    out_ref[...] = (mom_ref[...] + grad_ref[...].astype(F32)) - 0.1 * update
    for copy in sent:
        copy.wait_send()
    ring.finish()
    drain(sums_came.at[pl.ds(0, nc - 1)], n_ss)


def right_and_update(mom, grad, p, nz, nc):
    cols, rows = mom.shape
    rank = p.shape[0]
    half, wide = nz // 2, rank // nz
    thin = wide // 2
    whole = pl.BlockSpec(memory_space=pltpu.VMEM)
    return pl.pallas_call(
        lambda *refs: right_kernel(nz, nc, *refs),
        out_shape=(jax.ShapeDtypeStruct((cols, rows), F32), jax.ShapeDtypeStruct((wide, cols), F32)),
        in_specs=[whole] * 3,
        out_specs=(whole, whole),
        scratch_shapes=[
            pltpu.VMEM((cols, rows), BF16),
            pltpu.VMEM((nz, 2, thin, cols), F32),
            pltpu.VMEM((2, half, 2, thin, cols), BF16),
            pltpu.VMEM((2, half, 2, thin, cols), BF16),
            pltpu.VMEM((2, thin, cols), F32),
            pltpu.VMEM((nz, 2, thin, cols), BF16),
            pltpu.VMEM((rank, rows), BF16),
            pltpu.VMEM((wide, 128), F32),
            pltpu.VMEM((nc, wide, 128), F32),
            DMA((2, half, 2)), DMA((2, half, 2)), DMA((2, half, 2)), DMA((nz, 2)), DMA, DMA,
        ],
        compiler_params=pltpu.CompilerParams(
            collective_id=1, has_side_effects=True, vmem_limit_bytes=40 * 1024 * 1024),
        name="right_and_update",
    )(mom, grad, p)


def solution(mesh):
    nz, nc = mesh.shape["row"], mesh.shape["col"]

    def body(momentum, gradient, q_basis):
        mom, grad, q = momentum.T, gradient.T, q_basis.T
        w, gram = power_and_gram(mom, grad, q, nz, nc)
        p_low, p_out = solve(gram, w, w.shape[1] // nc)
        mom_next, q_next = right_and_update(mom, grad, p_low, nz, nc)
        return mom_next.T, p_out, q_next.T

    placed = (P("row", "col"), P("row", "col"), P("col", "row"))
    return jax.shard_map(
        body, mesh=mesh, in_specs=placed, out_specs=(P("row", "col"), P(("row", "col"), None), P("col", "row")),
        check_vma=False,
    )
```

```python
import jax
import jax.numpy as jnp
from jax import lax
from jax.experimental import pallas as pl
from jax.experimental.pallas import tpu as pltpu
from jax.sharding import PartitionSpec as P

HI = lax.Precision.HIGHEST
MESH = pl.DeviceIdType.MESH
F32, BF16 = jnp.float32, jnp.bfloat16
NB = 128
DMA = pltpu.SemaphoreType.DMA
NT = (((1,), (1,)), ((), ()))
TN = (((0,), (0,)), ((), ()))


def send(src, dst, send_sem, recv_sem, **where):
    copy = pltpu.make_async_remote_copy(
        src_ref=src, dst_ref=dst, send_sem=send_sem, recv_sem=recv_sem, device_id=where, device_id_type=MESH
    )
    copy.start()
    return copy


def drain(view, sem):
    pltpu.make_async_copy(view, view, sem).wait()


def greet(z, c, nz, nc):
    barrier = pltpu.get_barrier_semaphore()
    near = (1, 2, nz - 2, nz - 1)
    for step in near:
        pl.semaphore_signal(barrier, inc=1, device_id={"row": lax.rem(z + step, nz)}, device_id_type=MESH)

    @pl.loop(1, nc)
    def _(j):
        pl.semaphore_signal(barrier, inc=1, device_id={"col": lax.rem(c + j, nc)}, device_id_type=MESH)

    def met():
        pl.semaphore_wait(barrier, len(near) + nc - 1)

    return met


class Ring:
    def __init__(self, held, send_sems, recv_sems, z, nz):
        self.held, self.ss, self.rs = held, send_sems, recv_sems
        self.nz, self.half = nz, nz // 2
        self.rounds = self.half // 2
        self.to = [[lax.rem(z + step, nz) for step in (hops, nz - hops)] for hops in (1, 2)]
        self.sent, self.got = [], set()

    def arrived(self, slot, chunk):
        if slot != 0 and (slot, chunk) not in self.got:
            self.got.add((slot, chunk))
            drain(self.held.at[slot, chunk], self.rs.at[slot, chunk])

    def slots_arrived(self, *slots):
        for slot in slots:
            for chunk in (0, 1):
                self.arrived(slot % self.nz, chunk)

    def round(self, r):
        for hops in (2, 1):
            for chunk in (0, 1):
                for way in (0, 1):
                    src, dst = 2 * r, 2 * r + hops
                    if dst == self.half and chunk != way:
                        continue
                    if way:
                        src, dst = (self.nz - src) % self.nz, self.nz - dst
                    self.arrived(src, chunk)
                    self.sent.append(send(
                        self.held.at[src, chunk], self.held.at[dst, chunk],
                        self.ss.at[way, r, hops - 1, chunk], self.rs.at[dst, chunk], row=self.to[hops - 1][way]))

    def finish(self):
        for copy in self.sent:
            copy.wait_send()


def power_kernel(
    nz, nc, mom_ref, grad_ref, q_ref, w_out, g_ref,
    w_ref, mom, grad, blow, held, parts, came, shares, gpart, gcame, grow, gall,
    q_ss, q_rs, c_ss, c_rs, a_ss, a_rs, d_ss, d_rs, z_ss, z_rs, y_ss, y_rs, g_ss, g_rs, e_ss, e_rs, i_s,
):
    z, c = lax.axis_index("row"), lax.axis_index("col")
    chip, core = lax.div(c, 2), lax.rem(c, 2)
    partner = chip * 2 + 1 - core
    chips, half = nc // 2, nz // 2
    wide = q_ref.shape[0]
    thin = wide // 2
    copies = [pltpu.make_async_copy(q_ref.at[pl.ds(thin * chunk, thin)], held.at[0, chunk], i_s.at[chunk]) for chunk in (0, 1)]
    loads = [pltpu.make_async_copy(grad_ref, grad, i_s.at[2]), pltpu.make_async_copy(mom_ref, mom, i_s.at[3])]
    for copy in copies:
        copy.start()
    met = greet(z, c, nz, nc)
    for copy in loads:
        copy.start()
    rows = blow.shape[1]
    lanes = rows // 128
    for copy in copies:
        copy.wait()
    met()
    ring = Ring(held, q_ss, q_rs, z, nz)
    sides = [(t, (nz - t) % nz if t else half) for t in range(half)]

    def multiply(*pairs):
        slots = [slot for p in pairs for slot in sides[p]]
        ring.slots_arrived(*slots)
        lhs = jnp.concatenate([held[slot].reshape(wide, -1) for slot in slots], axis=0)
        prod = jnp.dot(lhs, blow[...], preferred_element_type=F32)
        for i, p in enumerate(pairs):
            pass_on(p, prod[2 * wide * i:2 * wide * (i + 1)])

    def pass_on(p, prod):
        for side in (0, 1):
            for piece in range(chips):
                s, l = piece // lanes, piece % lanes
                parts[p, side, piece] = prod[side * wide + 8 * s:side * wide + 8 * s + 8, 128 * l:128 * l + 128]
        came[p, c] = parts[p, core, chip]

        @pl.loop(1, nc)
        def _(j):
            to = lax.rem(c + j, nc)
            send(parts.at[p, lax.rem(to, 2), lax.div(to, 2)], came.at[p, c], c_ss.at[p], c_rs.at[p], col=to)

    def add_up(p):
        drain(came.at[p, pl.ds(0, nc - 1)], c_rs.at[p])
        shares[p, core, chip] = came[p].sum(axis=0)

        mine = shares.at[p, core, chip]
        if p in late:
            @pl.loop(1, nc)
            def _(j):
                send(mine, mine, a_ss.at[p], a_rs.at[p], col=lax.rem(c + j, nc))
        else:
            @pl.loop(1, chips)
            def _(j):
                send(mine, mine, a_ss.at[p], a_rs.at[p], col=lax.rem(chip + j, chips) * 2 + core)

    def cross(p):
        drain(shares.at[p, core, pl.ds(0, chips - 1)], a_rs.at[p])
        view = shares.at[p, core]
        send(view, view, d_ss.at[p], d_rs.at[p], col=partner)

    late = (half - 1, 0)
    groups = [(2 * r - 1, 2 * r) for r in range(1, ring.rounds)] + [late]
    ring.round(0)
    for copy in loads:
        copy.wait()
    blow[...] = (mom[...] + grad[...].astype(F32)).astype(BF16)
    for i in range(len(groups) + 2):
        if i + 1 < ring.rounds:
            ring.round(i + 1)
        if i < len(groups):
            multiply(*groups[i])
        if 1 <= i <= len(groups):
            for p in groups[i - 1]:
                add_up(p)
        if 2 <= i <= len(groups):
            for p in groups[i - 2]:
                cross(p)
    for p in range(half):
        if p in late:
            drain(came.at[p, pl.ds(0, nc - 1)], a_rs.at[p])
        else:
            drain(shares.at[p, core], d_rs.at[p])
    for p in range(half):
        for side in (0, 1):
            at = lax.rem(z + nz - sides[p][side], nz) * wide
            for piece in range(chips):
                s, l = piece // lanes, piece % lanes
                w_ref[pl.ds(pl.multiple_of(at + 8 * s, 8), 8), 128 * l:128 * l + 128] = shares[p, side, piece]

    w_copy = pltpu.make_async_copy(w_ref, w_out, i_s.at[0])
    w_copy.start()
    share = w_ref.shape[0] // nc
    mine = w_ref[pl.ds(pl.multiple_of(c * share, share), share), :]
    prod = lax.dot_general(mine, w_ref[...], NT, precision=HI, preferred_element_type=F32)
    glanes = prod.shape[1] // 128
    tall = share * glanes // nz
    for piece in range(nz):
        s, l = piece // glanes, piece % glanes
        gpart[piece] = prod[tall * s:tall * (s + 1), 128 * l:128 * l + 128]
    gcame[z] = gpart[z]

    @pl.loop(1, nz)
    def _(j):
        to = lax.rem(z + j, nz)
        send(gpart.at[to], gcame.at[z], z_ss, z_rs, row=to)

    drain(gcame.at[pl.ds(0, nz - 1)], z_rs)
    grow[z] = gcame[...].sum(axis=0)

    @pl.loop(1, nz)
    def _(j):
        to = lax.rem(z + j, nz)
        send(grow.at[z], grow.at[z], y_ss, y_rs, row=to)

    drain(grow.at[pl.ds(0, nz - 1)], y_rs)
    gall[core, chip] = grow[...]

    @pl.loop(1, chips)
    def _(j):
        to = lax.rem(chip + j, chips) * 2 + core
        mine = gall.at[core, chip]
        send(mine, mine, g_ss, g_rs, col=to)

    drain(gall.at[core, pl.ds(0, chips - 1)], g_rs)
    across = send(gall.at[core], gall.at[core], e_ss, e_rs, col=partner)
    w_copy.wait()
    ring.finish()
    for p in range(half):
        drain(came.at[p, pl.ds(0, nc - 1)], c_ss.at[p])
        if p in late:
            drain(came.at[p, pl.ds(0, nc - 1)], a_ss.at[p])
        else:
            drain(shares.at[p, core, pl.ds(0, chips - 1)], a_ss.at[p])
            drain(shares.at[p, core], d_ss.at[p])
    drain(gcame.at[pl.ds(0, nz - 1)], z_ss)
    drain(grow.at[pl.ds(0, nz - 1)], y_ss)
    drain(gall.at[core, pl.ds(0, chips - 1)], g_ss)
    across.wait()
    for other in range(nc):
        for piece in range(nz):
            s, l = piece // glanes, piece % glanes
            top = other * share + tall * s
            g_ref[top:top + tall, 128 * l:128 * l + 128] = gall[other % 2, other // 2, piece]


def power_and_gram(mom, grad, q, nz, nc):
    cols, rows = mom.shape
    wide = q.shape[0]
    rank, half, chips = wide * nz, nz // 2, nc // 2
    share = rank // nc
    tall = share * (rank // 128) // nz
    whole = pl.BlockSpec(memory_space=pltpu.VMEM)
    away = pl.BlockSpec(memory_space=pltpu.HBM)
    return pl.pallas_call(
        lambda *refs: power_kernel(nz, nc, *refs),
        out_shape=(jax.ShapeDtypeStruct((rank, rows), F32), jax.ShapeDtypeStruct((rank, rank), F32)),
        in_specs=[away] * 3,
        out_specs=(away, whole),
        scratch_shapes=[
            pltpu.VMEM((rank, rows), F32),
            pltpu.VMEM((cols, rows), F32),
            pltpu.VMEM((cols, rows), BF16),
            pltpu.VMEM((cols, rows), BF16),
            pltpu.VMEM((nz, 2, wide // 2, cols), BF16),
            pltpu.VMEM((half, 2, chips, 8, 128), F32),
            pltpu.VMEM((half, nc, 8, 128), F32),
            pltpu.VMEM((half, 2, chips, 8, 128), F32),
            pltpu.VMEM((nz, tall, 128), F32),
            pltpu.VMEM((nz, tall, 128), F32),
            pltpu.VMEM((nz, tall, 128), F32),
            pltpu.VMEM((2, chips, nz, tall, 128), F32),
            DMA((2, half // 2, 2, 2)), DMA((nz, 2)),
            DMA((half,)), DMA((half,)), DMA((half,)), DMA((half,)), DMA((half,)), DMA((half,)),
            DMA, DMA, DMA, DMA, DMA, DMA, DMA, DMA, DMA((4,)),
        ],
        compiler_params=pltpu.CompilerParams(
            collective_id=0, has_side_effects=True, vmem_limit_bytes=67043328),
        name="power_and_gram",
    )(mom, grad, q)


def sub_bcast(x, j):
    return jnp.broadcast_to(x[j:j + 1, :], x.shape)


def lane_bcast(x, j):
    return jnp.broadcast_to(x[:, j:j + 1], x.shape)


def diag_inverse(d_ref, inv_ref):
    n = NB // 8
    row = lax.broadcasted_iota(jnp.int32, (8, NB), 0)
    lane = lax.broadcasted_iota(jnp.int32, (8, NB), 1)
    for g in range(n):
        inv_ref[8 * g:8 * g + 8, :] = jnp.where(row + 8 * g == lane, 1.0, 0.0).astype(jnp.float32)
    for s in range(n):
        rd = d_ref[8 * s:8 * s + 8, :]
        ri = inv_ref[8 * s:8 * s + 8, :]
        c = [lane_bcast(rd, 8 * s + k) for k in range(8)]
        u = {}
        scale = []
        ud = []
        ui = []
        for j in range(8):
            rs = lax.rsqrt(sub_bcast(c[j], j))
            scale.append(rs)
            lj = jnp.where(row > j, c[j] * rs, 0.0)
            for k in range(j + 1, 8):
                u[j, k] = sub_bcast(c[k], j) * rs
                c[k] = c[k] - lj * u[j, k]
            ud.append(sub_bcast(rd, j) * rs)
            ui.append(sub_bcast(ri, j) * rs)
            rd = rd - lj * ud[j]
            ri = ri - lj * ui[j]
        out = ui[7]
        for j in range(7):
            out = jnp.where(row == j, ui[j], out)
        inv_ref[8 * s:8 * s + 8, :] = out
        for g in range(s + 1, n):
            rd = d_ref[8 * g:8 * g + 8, :]
            ri = inv_ref[8 * g:8 * g + 8, :]
            c = [lane_bcast(rd, 8 * s + k) for k in range(8)]
            for j in range(8):
                lj = c[j] * scale[j]
                for k in range(j + 1, 8):
                    c[k] = c[k] - lj * u[j, k]
                rd = rd - lj * ud[j]
                ri = ri - lj * ui[j]
            d_ref[8 * g:8 * g + 8, :] = rd
            inv_ref[8 * g:8 * g + 8, :] = ri


def solve_kernel(g_ref, w_ref, low_ref, p_ref, a, d, inv, pt):
    rank = w_ref.shape[0]
    rows = w_ref.shape[1]
    blocks = rank // NB
    a[:, :rank] = g_ref[...]
    a[:, rank:] = w_ref[...]

    def step(b, carry):
        at = pl.multiple_of(b * NB, NB)
        d[...] = a[pl.ds(at, NB), pl.ds(at, NB)]
        diag_inverse(d, inv)
        for bb in range(blocks):
            @pl.when(b == bb)
            def _():
                lo, hi = bb * NB, (bb + 1) * NB
                y = jnp.dot(inv[...], a[lo:hi, hi:], precision=HI, preferred_element_type=jnp.float32)
                x = y[:, rank - hi:]
                a[lo:hi, rank:] = x
                if bb < blocks - 1:
                    ut = y[:, :rank - hi].T
                    a[hi:rank, hi:] = a[hi:rank, hi:] - jnp.dot(
                        ut, y, precision=HI, preferred_element_type=jnp.float32)
        return carry

    lax.fori_loop(0, blocks, step, 0)
    full = a[:, rank:]
    low_ref[...] = full.astype(jnp.bfloat16)
    pt[...] = full.T
    share = p_ref.shape[0]
    mine = lax.axis_index("col") * share
    p_ref[...] = pt[pl.ds(pl.multiple_of(mine, share), share), :]


def solve(gram, w, share):
    rank, rows = w.shape
    whole = pl.BlockSpec(memory_space=pltpu.VMEM)
    return pl.pallas_call(
        solve_kernel,
        out_shape=(jax.ShapeDtypeStruct((rank, rows), jnp.bfloat16), jax.ShapeDtypeStruct((share, rank), jnp.float32)),
        in_specs=[whole, whole],
        out_specs=(whole, whole),
        scratch_shapes=[
            pltpu.VMEM((rank, rank + rows), jnp.float32),
            pltpu.VMEM((NB, NB), jnp.float32),
            pltpu.VMEM((NB, NB), jnp.float32),
            pltpu.VMEM((rows, rank), jnp.float32),
        ],
        compiler_params=pltpu.CompilerParams(vmem_limit_bytes=40 * 1024 * 1024),
        name="solve",
    )(gram, w)


def right_kernel(
    nz, nc, mom_ref, grad_ref, p_ref, out_ref, q_ref,
    blow, part, leaf, leaf_came, stem, stem_came, cols, held, turned, sums, sums_came,
    l_ss, l_rs, r_ss, r_rs, q_ss, q_rs, n_ss, n_rs,
):
    z, c = lax.axis_index("row"), lax.axis_index("col")
    half = nz // 2
    met = greet(z, c, nz, nc)
    blow[...] = (mom_ref[...] + grad_ref[...].astype(F32)).astype(BF16)
    wide = q_ref.shape[0]
    thin = wide // 2
    prod = lax.dot_general(p_ref[...], blow[...], NT, preferred_element_type=F32)
    for block in range(nz):
        for chunk in (0, 1):
            at = block * wide + chunk * thin
            part[block, chunk] = prod[at:at + thin, :]
    met()
    to = [[lax.rem(z + step, nz) for step in (nz - hops, hops)] for hops in (1, 2)]
    sent = []

    def own(way, far, chunk):
        return part[lax.rem(z + (far if way else nz - far), nz), chunk]

    def inbound(came, sems, way, k, chunk):
        drain(came.at[way, k, chunk], sems.at[way, k, chunk])
        return came[way, k, chunk].astype(F32)

    def outbound(value, held_out, came, send_sems, recv_sems, way, k, chunk, hops):
        held_out[way, k, chunk] = value.astype(BF16)
        sent.append(send(
            held_out.at[way, k, chunk], came.at[way, k, chunk],
            send_sems.at[way, k, chunk], recv_sems.at[way, k, chunk], row=to[hops - 1][way]))

    for far in range(half, 0, -2):
        k = far // 2
        for chunk in (0, 1):
            for way in (0, 1):
                if far == half and chunk != way:
                    continue
                value = own(way, far, chunk)
                if far < half:
                    value = value + inbound(leaf_came, l_rs, way, k, chunk)
                if far < half - 2 or (far < half and chunk == way):
                    value = value + inbound(stem_came, r_rs, way, k, chunk)
                outbound(value, stem, stem_came, r_ss, r_rs, way, k - 1, chunk, 2)
        for chunk in (0, 1):
            for way in (0, 1):
                outbound(own(way, far - 1, chunk), leaf, leaf_came, l_ss, l_rs, way, k - 1, chunk, 1)
    for chunk in (0, 1):
        value = part[z, chunk]
        for way in (0, 1):
            value = value + inbound(leaf_came, l_rs, way, 0, chunk) + inbound(stem_came, r_rs, way, 0, chunk)
        cols[chunk] = value
        held[0, chunk] = value.astype(BF16)
    ring = Ring(held, q_ss, q_rs, z, nz)
    ring.round(0)
    value = cols[...].reshape(wide, -1)
    sums[...] = jnp.broadcast_to(jnp.sum(value * value, axis=1, keepdims=True), (wide, 128))
    sums_came[c] = sums[...]

    @pl.loop(1, nc)
    def _(j):
        send(sums, sums_came.at[c], n_ss, n_rs, col=lax.rem(c + j, nc))

    for slot in range(nz):
        at = lax.rem(z + nz - slot, nz) * wide
        turned[wide * slot:wide * (slot + 1), :] = p_ref[pl.ds(pl.multiple_of(at, wide), wide), :]
    for r in range(1, ring.rounds):
        ring.round(r)
        if r == ring.rounds - 1:
            drain(sums_came.at[pl.ds(0, nc - 1)], n_rs)
            norms = jnp.sqrt(jnp.sum(sums_came[...], axis=0)[:, :1] + 1e-06)
            q_ref[...] = value / norms
    ring.slots_arrived(*range(nz))
    right = held[...].reshape(nz * wide, -1)
    update = lax.dot_general(right, turned[...], TN, preferred_element_type=F32)
    out_ref[...] = (mom_ref[...] + grad_ref[...].astype(F32)) - 0.1 * update
    for copy in sent:
        copy.wait_send()
    ring.finish()
    drain(sums_came.at[pl.ds(0, nc - 1)], n_ss)


def right_and_update(mom, grad, p, nz, nc):
    cols, rows = mom.shape
    rank = p.shape[0]
    half, wide = nz // 2, rank // nz
    thin = wide // 2
    whole = pl.BlockSpec(memory_space=pltpu.VMEM)
    return pl.pallas_call(
        lambda *refs: right_kernel(nz, nc, *refs),
        out_shape=(jax.ShapeDtypeStruct((cols, rows), F32), jax.ShapeDtypeStruct((wide, cols), F32)),
        in_specs=[whole] * 3,
        out_specs=(whole, whole),
        scratch_shapes=[
            pltpu.VMEM((cols, rows), BF16),
            pltpu.VMEM((nz, 2, thin, cols), F32),
            pltpu.VMEM((2, half // 2, 2, thin, cols), BF16),
            pltpu.VMEM((2, half // 2, 2, thin, cols), BF16),
            pltpu.VMEM((2, half // 2, 2, thin, cols), BF16),
            pltpu.VMEM((2, half // 2, 2, thin, cols), BF16),
            pltpu.VMEM((2, thin, cols), F32),
            pltpu.VMEM((nz, 2, thin, cols), BF16),
            pltpu.VMEM((rank, rows), BF16),
            pltpu.VMEM((wide, 128), F32),
            pltpu.VMEM((nc, wide, 128), F32),
            DMA((2, half // 2, 2)), DMA((2, half // 2, 2)), DMA((2, half // 2, 2)), DMA((2, half // 2, 2)),
            DMA((2, half // 2, 2, 2)), DMA((nz, 2)), DMA, DMA,
        ],
        compiler_params=pltpu.CompilerParams(
            collective_id=1, has_side_effects=True, vmem_limit_bytes=40 * 1024 * 1024),
        name="right_and_update",
    )(mom, grad, p)


def solution(mesh):
    nz, nc = mesh.shape["row"], mesh.shape["col"]

    def body(momentum, gradient, q_basis):
        mom, grad, q = momentum.T, gradient.T, q_basis.T
        w, gram = power_and_gram(mom, grad, q, nz, nc)
        p_low, p_out = solve(gram, w, w.shape[1] // nc)
        mom_next, q_next = right_and_update(mom, grad, p_low, nz, nc)
        return mom_next.T, p_out, q_next.T

    placed = (P("row", "col"), P("row", "col"), P("col", "row"))
    return jax.shard_map(
        body, mesh=mesh, in_specs=placed, out_specs=(P("row", "col"), P(("row", "col"), None), P("col", "row")),
        check_vma=False,
    )
```

```python
from types import SimpleNamespace

import jax
import jax.numpy as jnp
from jax import lax
from jax.experimental import pallas as pl
from jax.experimental.pallas import tpu as pltpu
from jax.sharding import PartitionSpec as P

HI = lax.Precision.HIGHEST
MESH = pl.DeviceIdType.MESH
F32, BF16 = jnp.float32, jnp.bfloat16
NB = 128
DMA = pltpu.SemaphoreType.DMA
NT = (((1,), (1,)), ((), ()))
TN = (((0,), (0,)), ((), ()))


def send(src, dst, send_sem, recv_sem, **where):
    copy = pltpu.make_async_remote_copy(
        src_ref=src, dst_ref=dst, send_sem=send_sem, recv_sem=recv_sem, device_id=where, device_id_type=MESH
    )
    copy.start()
    return copy


def drain(view, sem):
    pltpu.make_async_copy(view, view, sem).wait()


def greet(z, c, nz, nc):
    barrier = pltpu.get_barrier_semaphore()
    near = (1, 2, nz - 2, nz - 1)
    for step in near:
        pl.semaphore_signal(barrier, inc=1, device_id={"row": lax.rem(z + step, nz)}, device_id_type=MESH)

    @pl.loop(1, nc)
    def _(j):
        pl.semaphore_signal(barrier, inc=1, device_id={"col": lax.rem(c + j, nc)}, device_id_type=MESH)

    def met():
        pl.semaphore_wait(barrier, len(near) + nc - 1)

    return met


class Ring:
    def __init__(self, held, send_sems, recv_sems, z, nz):
        self.held, self.ss, self.rs = held, send_sems, recv_sems
        self.nz, self.half = nz, nz // 2
        self.rounds = self.half // 2
        self.to = [[lax.rem(z + step, nz) for step in (hops, nz - hops)] for hops in (1, 2)]
        self.sent, self.got = [], set()

    def arrived(self, slot, chunk):
        if slot != 0 and (slot, chunk) not in self.got:
            self.got.add((slot, chunk))
            drain(self.held.at[slot, chunk], self.rs.at[slot, chunk])

    def slots_arrived(self, *slots):
        for slot in slots:
            for chunk in (0, 1):
                self.arrived(slot % self.nz, chunk)

    def round(self, r):
        for hops in (2, 1):
            for chunk in (0, 1):
                for way in (0, 1):
                    src, dst = 2 * r, 2 * r + hops
                    if dst == self.half and chunk != way:
                        continue
                    if way:
                        src, dst = (self.nz - src) % self.nz, self.nz - dst
                    self.arrived(src, chunk)
                    self.sent.append(send(
                        self.held.at[src, chunk], self.held.at[dst, chunk],
                        self.ss.at[way, r, hops - 1, chunk], self.rs.at[dst, chunk], row=self.to[hops - 1][way]))

    def finish(self):
        for copy in self.sent:
            copy.wait_send()


def sub_bcast(x, j):
    return jnp.broadcast_to(x[j:j + 1, :], x.shape)


def lane_bcast(x, j):
    return jnp.broadcast_to(x[:, j:j + 1], x.shape)


def diag_inverse(d_ref, inv_ref):
    n = NB // 8
    row = lax.broadcasted_iota(jnp.int32, (8, NB), 0)
    lane = lax.broadcasted_iota(jnp.int32, (8, NB), 1)
    for g in range(n):
        inv_ref[8 * g:8 * g + 8, :] = jnp.where(row + 8 * g == lane, 1.0, 0.0).astype(jnp.float32)
    for s in range(n):
        rd = d_ref[8 * s:8 * s + 8, :]
        ri = inv_ref[8 * s:8 * s + 8, :]
        c = [lane_bcast(rd, 8 * s + k) for k in range(8)]
        u = {}
        scale = []
        ud = []
        ui = []
        for j in range(8):
            rs = lax.rsqrt(sub_bcast(c[j], j))
            scale.append(rs)
            lj = jnp.where(row > j, c[j] * rs, 0.0)
            for k in range(j + 1, 8):
                u[j, k] = sub_bcast(c[k], j) * rs
                c[k] = c[k] - lj * u[j, k]
            ud.append(sub_bcast(rd, j) * rs)
            ui.append(sub_bcast(ri, j) * rs)
            rd = rd - lj * ud[j]
            ri = ri - lj * ui[j]
        out = ui[7]
        for j in range(7):
            out = jnp.where(row == j, ui[j], out)
        inv_ref[8 * s:8 * s + 8, :] = out
        for g in range(s + 1, n):
            rd = d_ref[8 * g:8 * g + 8, :]
            ri = inv_ref[8 * g:8 * g + 8, :]
            c = [lane_bcast(rd, 8 * s + k) for k in range(8)]
            for j in range(8):
                lj = c[j] * scale[j]
                for k in range(j + 1, 8):
                    c[k] = c[k] - lj * u[j, k]
                rd = rd - lj * ud[j]
                ri = ri - lj * ui[j]
            d_ref[8 * g:8 * g + 8, :] = rd
            inv_ref[8 * g:8 * g + 8, :] = ri


def scratch_of(nz, nc, cols, rows, wide):
    rank, half, chips = wide * nz, nz // 2, nc // 2
    thin, quarter, hi = wide // 2, nz // 4, rank // 2
    tall = (rank // nc) * (rank // 128) // nz
    win = window_rows(cols, nz)
    vm = pltpu.VMEM
    return dict(
        mom=vm((cols, rows), F32), grad=vm((cols, rows), BF16), blow=vm((cols, rows), BF16),
        held=vm((nz, 2, thin, cols), BF16),
        parts=vm((half, 2, chips, 8, 128), F32), came=vm((half, nc, 8, 128), F32),
        shares=vm((half, 2, chips, 8, 128), F32), w=vm((rank, rows), F32),
        gpart=vm((nz, tall, 128), F32), gcame=vm((nz, tall, 128), F32), grow=vm((nz, tall, 128), F32),
        gall=vm((2, chips, nz, tall, 128), F32),
        a=vm((rank, 2 * rank), F32), d=vm((NB, NB), F32), inv=vm((NB, NB), F32),
        y=vm((2, cols, hi), F32),
        leaf_came=vm((2, quarter, 2, win, hi), F32), stem=vm((2, quarter, 2, win, hi), F32),
        stem_came=vm((2, quarter, 2, win, hi), F32), own=vm((2, win, hi), F32),
        right=vm((nz, 2, win, hi), BF16), r32=vm((cols, rank), F32),
        plow=vm((rank, rows), BF16), pt=vm((rows, rank), F32),
        sz=vm((nz, rank // 128, 128), F32), sx=vm((nc, rank // 128, 128), F32),
        q_ss=DMA((2, quarter, 2, 2)), q_rs=DMA((nz, 2)),
        c_ss=DMA((half,)), c_rs=DMA((half,)), a_ss=DMA((half,)), a_rs=DMA((half,)), d_ss=DMA((half,)), d_rs=DMA((half,)),
        z_ss=DMA, z_rs=DMA, y_ss=DMA, y_rs=DMA, g_ss=DMA, g_rs=DMA, e_ss=DMA, e_rs=DMA,
        l_ss=DMA((2, quarter, 2)), l_rs=DMA((2, quarter, 2)), r_ss=DMA((2, quarter, 2)), r_rs=DMA((2, quarter, 2)),
        p_ss=DMA((2, quarter, 2, 2)), p_rs=DMA((nz, 2)),
        n_ss=DMA, n_rs=DMA, m_ss=DMA, m_rs=DMA, i_s=DMA((4,)),
    )


def window_rows(cols, nz):
    return -(-(cols // nz) // 8) * 8


def window_start(i, cols, nz):
    return pl.multiple_of(lax.div(i * (cols // nz), 8) * 8, 8)


def split3(x):
    one = x.astype(BF16)
    rest = x - one.astype(F32)
    two = rest.astype(BF16)
    return one, two, (rest - two.astype(F32)).astype(BF16)


def kernel(nz, nc, mom_hbm, grad_hbm, q_hbm, m_out, p_out, q_out, s):
    z, c = lax.axis_index("row"), lax.axis_index("col")
    chip, core = lax.div(c, 2), lax.rem(c, 2)
    partner = chip * 2 + 1 - core
    chips, half = nc // 2, nz // 2
    wide = q_hbm.shape[0]
    thin = wide // 2
    cols, rows = s.blow.shape
    rank = wide * nz
    hi = rank // 2
    lanes = rows // 128

    def others(count):
        return pl.ds(0, count - 1)

    copies = [
        pltpu.make_async_copy(q_hbm.at[pl.ds(thin * chunk, thin)], s.held.at[0, chunk], s.i_s.at[chunk])
        for chunk in (0, 1)
    ]
    loads = [pltpu.make_async_copy(grad_hbm, s.grad, s.i_s.at[2]), pltpu.make_async_copy(mom_hbm, s.mom, s.i_s.at[3])]
    for copy in copies:
        copy.start()
    met = greet(z, c, nz, nc)
    for copy in loads:
        copy.start()
    for copy in copies:
        copy.wait()
    met()

    ring = Ring(s.held, s.q_ss, s.q_rs, z, nz)
    sides = [(t, (nz - t) % nz if t else half) for t in range(half)]
    late = (half - 1, 0)
    groups = [(2 * r - 1, 2 * r) for r in range(1, ring.rounds)] + [late]

    def multiply(*pairs):
        slots = [slot for p in pairs for slot in sides[p]]
        ring.slots_arrived(*slots)
        lhs = jnp.concatenate([s.held[slot].reshape(wide, -1) for slot in slots], axis=0)
        prod = jnp.dot(lhs, s.blow[...], preferred_element_type=F32)
        for i, p in enumerate(pairs):
            pass_on(p, prod[2 * wide * i:2 * wide * (i + 1)])

    def pass_on(p, prod):
        for side in (0, 1):
            for piece in range(chips):
                i, l = piece // lanes, piece % lanes
                s.parts[p, side, piece] = prod[side * wide + 8 * i:side * wide + 8 * i + 8, 128 * l:128 * l + 128]
        s.came[p, c] = s.parts[p, core, chip]

        @pl.loop(1, nc)
        def _(j):
            to = lax.rem(c + j, nc)
            send(s.parts.at[p, lax.rem(to, 2), lax.div(to, 2)], s.came.at[p, c], s.c_ss.at[p], s.c_rs.at[p], col=to)

    def add_up(p):
        drain(s.came.at[p, others(nc)], s.c_rs.at[p])
        s.shares[p, core, chip] = s.came[p].sum(axis=0)
        mine = s.shares.at[p, core, chip]
        if p in late:
            @pl.loop(1, nc)
            def _(j):
                send(mine, mine, s.a_ss.at[p], s.a_rs.at[p], col=lax.rem(c + j, nc))
        else:
            @pl.loop(1, chips)
            def _(j):
                send(mine, mine, s.a_ss.at[p], s.a_rs.at[p], col=lax.rem(chip + j, chips) * 2 + core)

    def cross(p):
        drain(s.shares.at[p, core, others(chips)], s.a_rs.at[p])
        view = s.shares.at[p, core]
        send(view, view, s.d_ss.at[p], s.d_rs.at[p], col=partner)

    ring.round(0)
    for copy in loads:
        copy.wait()
    s.blow[...] = (s.mom[...] + s.grad[...].astype(F32)).astype(BF16)
    for i in range(len(groups)):
        if i + 1 < ring.rounds:
            ring.round(i + 1)
        multiply(*groups[i])
        if i >= 2:
            for p in groups[i - 2]:
                add_up(p)
    for p in groups[-2]:
        add_up(p)
    for p in groups[0]:
        cross(p)
    for p in late:
        add_up(p)
    for group in groups[1:-1]:
        for p in group:
            cross(p)
    for p in range(half):
        if p in late:
            drain(s.came.at[p, others(nc)], s.a_rs.at[p])
        else:
            drain(s.shares.at[p, core], s.d_rs.at[p])
    for p in range(half):
        for side in (0, 1):
            at = lax.rem(z + nz - sides[p][side], nz) * wide
            for piece in range(chips):
                i, l = piece // lanes, piece % lanes
                s.w[pl.ds(pl.multiple_of(at + 8 * i, 8), 8), 128 * l:128 * l + 128] = s.shares[p, side, piece]

    share = rank // nc
    mine = s.w[pl.ds(pl.multiple_of(c * share, share), share), :]
    prod = lax.dot_general(mine, s.w[...], NT, precision=HI, preferred_element_type=F32)
    glanes = rank // 128
    tall = share * glanes // nz
    for piece in range(nz):
        i, l = piece // glanes, piece % glanes
        s.gpart[piece] = prod[tall * i:tall * (i + 1), 128 * l:128 * l + 128]
    s.gcame[z] = s.gpart[z]

    @pl.loop(1, nz)
    def _(j):
        to = lax.rem(z + j, nz)
        send(s.gpart.at[to], s.gcame.at[z], s.z_ss, s.z_rs, row=to)

    pieces = split3(s.w[...])
    for chunk in (0, 1):
        s.y[chunk] = sum(
            lax.dot_general(s.blow[...], piece[hi * chunk:hi * (chunk + 1)], NT, preferred_element_type=F32)
            for piece in reversed(pieces)
        )

    drain(s.gcame.at[others(nz)], s.z_rs)
    s.grow[z] = s.gcame[...].sum(axis=0)

    @pl.loop(1, nz)
    def _(j):
        send(s.grow.at[z], s.grow.at[z], s.y_ss, s.y_rs, row=lax.rem(z + j, nz))

    win = window_rows(cols, nz)
    to = [[lax.rem(z + step, nz) for step in (nz - hops, hops)] for hops in (1, 2)]

    def share_of(i, chunk):
        return s.y.at[chunk, pl.ds(window_start(i, cols, nz), win), :]

    def far_one(way, far):
        return lax.rem(z + (far if way else nz - far), nz)

    def inbound(came, sems, way, k, chunk):
        drain(came.at[way, k, chunk], sems.at[way, k, chunk])
        return came[way, k, chunk]

    def sum_round(far):
        k = far // 2
        for chunk in (0, 1):
            for way in (0, 1):
                if far == half and chunk != way:
                    continue
                value = share_of(far_one(way, far), chunk)[...]
                if far < half:
                    value = value + inbound(s.leaf_came, s.l_rs, way, k, chunk)
                if far < half - 2 or (far < half and chunk == way):
                    value = value + inbound(s.stem_came, s.r_rs, way, k, chunk)
                s.stem[way, k - 1, chunk] = value
                send(s.stem.at[way, k - 1, chunk], s.stem_came.at[way, k - 1, chunk],
                     s.r_ss.at[way, k - 1, chunk], s.r_rs.at[way, k - 1, chunk], row=to[1][way])
        for chunk in (0, 1):
            for way in (0, 1):
                send(share_of(far_one(way, far - 1), chunk), s.leaf_came.at[way, k - 1, chunk],
                     s.l_ss.at[way, k - 1, chunk], s.l_rs.at[way, k - 1, chunk], row=to[0][way])

    sum_round(half)
    drain(s.grow.at[others(nz)], s.y_rs)
    s.gall[core, chip] = s.grow[...]

    @pl.loop(1, chips)
    def _(j):
        mine = s.gall.at[core, chip]
        send(mine, mine, s.g_ss, s.g_rs, col=lax.rem(chip + j, chips) * 2 + core)

    row = lax.broadcasted_iota(jnp.int32, (NB, rank), 0)
    lane = lax.broadcasted_iota(jnp.int32, (NB, rank), 1)
    for b in range(rank // NB):
        s.a[NB * b:NB * (b + 1), rank:] = jnp.where(row + NB * b == lane, 1.0, 0.0).astype(F32)
    sum_round(half - 2)
    drain(s.gall.at[core, others(chips)], s.g_rs)
    across = send(s.gall.at[core], s.gall.at[core], s.e_ss, s.e_rs, col=partner)
    across.wait()
    for other in range(nc):
        for piece in range(nz):
            i, l = piece // glanes, piece % glanes
            top = other * share + tall * i
            s.a[top:top + tall, 128 * l:128 * l + 128] = s.gall[other % 2, other // 2, piece]

    sum_round(half - 4)

    blocks = rank // NB

    def step(b, carry):
        at = pl.multiple_of(b * NB, NB)
        s.d[...] = s.a[pl.ds(at, NB), pl.ds(at, NB)]
        diag_inverse(s.d, s.inv)
        for bb in range(blocks):
            @pl.when(b == bb)
            def _():
                low, top = bb * NB, (bb + 1) * NB
                prod = jnp.dot(s.inv[...], s.a[low:top, top:rank + top], precision=HI, preferred_element_type=F32)
                s.a[low:top, rank:rank + top] = prod[:, rank - top:]
                if bb < blocks - 1:
                    ut = prod[:, :rank - top].T
                    s.a[top:rank, top:rank + top] = s.a[top:rank, top:rank + top] - jnp.dot(
                        ut, prod, precision=HI, preferred_element_type=F32)
                if bb == 1:
                    for far in range(half - 6, 0, -2):
                        sum_round(far)
        return carry

    lax.fori_loop(0, blocks, step, 0)

    for chunk in (0, 1):
        value = share_of(z, chunk)[...]
        for way in (0, 1):
            value = value + inbound(s.leaf_came, s.l_rs, way, 0, chunk) + inbound(s.stem_came, s.r_rs, way, 0, chunk)
        s.own[chunk] = value
    right = sum(
        lax.dot_general(s.own[chunk], s.a[:, rank + hi * chunk:rank + hi * (chunk + 1)], NT,
                        precision=HI, preferred_element_type=F32)
        for chunk in (0, 1)
    )
    before = lax.rem(z + nz - 1, nz)
    seen = jnp.where(z == 0, 0, window_start(before, cols, nz) + win - window_start(z, cols, nz))
    fresh = lax.broadcasted_iota(jnp.int32, right.shape, 0) >= seen
    squares = jnp.sum(jnp.where(fresh, right * right, 0.0), axis=0, keepdims=True)
    for l in range(glanes):
        s.sz[z, l:l + 1, :] = squares[:, 128 * l:128 * l + 128]

    @pl.loop(1, nz)
    def _(j):
        send(s.sz.at[z], s.sz.at[z], s.n_ss, s.n_rs, row=lax.rem(z + j, nz))

    for chunk in (0, 1):
        s.right[0, chunk] = right[:, hi * chunk:hi * (chunk + 1)].astype(BF16)
    gather = Ring(s.right, s.p_ss, s.p_rs, z, nz)
    gather.round(0)

    p = jnp.dot(s.a[:, rank:], s.w[...], precision=HI, preferred_element_type=F32)
    s.plow[...] = p.astype(BF16)
    s.pt[...] = p.T
    out = p_out.shape[0]
    p_out[...] = s.pt[pl.ds(pl.multiple_of(c * out, out), out), :]

    for r in range(1, gather.rounds - 1):
        gather.round(r)
    drain(s.sz.at[others(nz)], s.n_rs)
    s.sx[c] = s.sz[...].sum(axis=0)

    @pl.loop(1, nc)
    def _(j):
        send(s.sx.at[c], s.sx.at[c], s.m_ss, s.m_rs, col=lax.rem(c + j, nc))

    gather.round(gather.rounds - 1)
    drain(s.sx.at[others(nc)], s.m_rs)
    total = s.sx[...].sum(axis=0)
    total = jnp.concatenate([total[l:l + 1, :] for l in range(glanes)], axis=1)
    pick = lax.broadcasted_iota(jnp.int32, (wide, rank), 1) == lax.broadcasted_iota(jnp.int32, (wide, rank), 0) + z * wide
    norms = jnp.sqrt(jnp.sum(jnp.where(pick, total, 0.0), axis=1, keepdims=True) + 1e-06)
    gather.slots_arrived(*range(nz))
    for slot in range(nz):
        at = window_start(lax.rem(z + nz - slot, nz), cols, nz)
        for chunk in (0, 1):
            s.r32[pl.ds(at, win), hi * chunk:hi * (chunk + 1)] = s.right[slot, chunk].astype(F32)
    low = s.r32[...].astype(BF16)
    update = jnp.dot(low, s.plow[...], preferred_element_type=F32)
    m_out[...] = (s.mom[...] + s.grad[...].astype(F32)) - 0.1 * update
    q_out[...] = lax.dot_general(jnp.where(pick, 1.0, 0.0).astype(BF16), low, NT, preferred_element_type=F32) / norms

    ring.finish()
    gather.finish()
    for p in range(half):
        drain(s.came.at[p, others(nc)], s.c_ss.at[p])
        if p in late:
            drain(s.came.at[p, others(nc)], s.a_ss.at[p])
        else:
            drain(s.shares.at[p, core, others(chips)], s.a_ss.at[p])
            drain(s.shares.at[p, core], s.d_ss.at[p])
    drain(s.gcame.at[others(nz)], s.z_ss)
    drain(s.grow.at[others(nz)], s.y_ss)
    drain(s.gall.at[core, others(chips)], s.g_ss)
    drain(s.sz.at[others(nz)], s.n_ss)
    drain(s.sx.at[others(nc)], s.m_ss)
    for way in (0, 1):
        for k in range(half // 2):
            for chunk in (0, 1):
                drain(s.leaf_came.at[way, k, chunk], s.l_ss.at[way, k, chunk])
                if k < half // 2 - 1 or chunk == way:
                    drain(s.stem_came.at[way, k, chunk], s.r_ss.at[way, k, chunk])


def run(mom, grad, q, nz, nc):
    cols, rows = mom.shape
    wide = q.shape[0]
    rank = wide * nz
    scratch = scratch_of(nz, nc, cols, rows, wide)
    names = list(scratch)
    whole = pl.BlockSpec(memory_space=pltpu.VMEM)
    return pl.pallas_call(
        lambda *refs: kernel(nz, nc, *refs[:6], SimpleNamespace(**dict(zip(names, refs[6:])))),
        out_shape=(
            jax.ShapeDtypeStruct((cols, rows), F32),
            jax.ShapeDtypeStruct((rows // nc, rank), F32),
            jax.ShapeDtypeStruct((wide, cols), F32),
        ),
        in_specs=[pl.BlockSpec(memory_space=pltpu.HBM)] * 3,
        out_specs=(whole,) * 3,
        scratch_shapes=list(scratch.values()),
        compiler_params=pltpu.CompilerParams(collective_id=0, has_side_effects=True, vmem_limit_bytes=67043328),
        name="dion",
    )(mom, grad, q)


def solution(mesh):
    nz, nc = mesh.shape["row"], mesh.shape["col"]

    def body(momentum, gradient, q_basis):
        mom_next, p_out, q_next = run(momentum.T, gradient.T, q_basis.T, nz, nc)
        return mom_next.T, p_out, q_next.T

    placed = (P("row", "col"), P("row", "col"), P("col", "row"))
    return jax.shard_map(
        body, mesh=mesh, in_specs=placed, out_specs=(P("row", "col"), P(("row", "col"), None), P("col", "row")),
        check_vma=False,
    )
```

```python
from types import SimpleNamespace

import jax
import jax.numpy as jnp
from jax import lax
from jax.experimental import pallas as pl
from jax.experimental.pallas import tpu as pltpu
from jax.sharding import PartitionSpec as P

HI = lax.Precision.HIGHEST
MESH = pl.DeviceIdType.MESH
F32, BF16 = jnp.float32, jnp.bfloat16
NB = 128
DMA = pltpu.SemaphoreType.DMA
NT = (((1,), (1,)), ((), ()))
TN = (((0,), (0,)), ((), ()))


def send(src, dst, send_sem, recv_sem, **where):
    copy = pltpu.make_async_remote_copy(
        src_ref=src, dst_ref=dst, send_sem=send_sem, recv_sem=recv_sem, device_id=where, device_id_type=MESH
    )
    copy.start()
    return copy


def drain(view, sem):
    pltpu.make_async_copy(view, view, sem).wait()


def greet(z, c, nz, nc):
    barrier = pltpu.get_barrier_semaphore()
    near = (1, 2, nz - 2, nz - 1)
    for step in near:
        pl.semaphore_signal(barrier, inc=1, device_id={"row": lax.rem(z + step, nz)}, device_id_type=MESH)

    @pl.loop(1, nc)
    def _(j):
        pl.semaphore_signal(barrier, inc=1, device_id={"col": lax.rem(c + j, nc)}, device_id_type=MESH)

    def met():
        pl.semaphore_wait(barrier, len(near) + nc - 1)

    return met


class Ring:
    def __init__(self, held, send_sems, recv_sems, z, nz):
        self.held, self.ss, self.rs = held, send_sems, recv_sems
        self.nz, self.half = nz, nz // 2
        self.rounds = self.half // 2
        self.to = [[lax.rem(z + step, nz) for step in (hops, nz - hops)] for hops in (1, 2)]
        self.sent, self.got = [], set()

    def arrived(self, slot, chunk):
        if slot != 0 and (slot, chunk) not in self.got:
            self.got.add((slot, chunk))
            drain(self.held.at[slot, chunk], self.rs.at[slot, chunk])

    def slots_arrived(self, *slots):
        for slot in slots:
            for chunk in (0, 1):
                self.arrived(slot % self.nz, chunk)

    def round(self, r):
        for hops in (2, 1):
            for chunk in (0, 1):
                for way in (0, 1):
                    src, dst = 2 * r, 2 * r + hops
                    if dst == self.half and chunk != way:
                        continue
                    if way:
                        src, dst = (self.nz - src) % self.nz, self.nz - dst
                    self.arrived(src, chunk)
                    self.sent.append(send(
                        self.held.at[src, chunk], self.held.at[dst, chunk],
                        self.ss.at[way, r, hops - 1, chunk], self.rs.at[dst, chunk], row=self.to[hops - 1][way]))

    def finish(self):
        for copy in self.sent:
            copy.wait_send()


def sub_bcast(x, j):
    return jnp.broadcast_to(x[j:j + 1, :], x.shape)


def lane_bcast(x, j):
    return jnp.broadcast_to(x[:, j:j + 1], x.shape)


def diag_inverse(d_ref, inv_ref):
    n = NB // 8
    row = lax.broadcasted_iota(jnp.int32, (8, NB), 0)
    lane = lax.broadcasted_iota(jnp.int32, (8, NB), 1)
    for g in range(n):
        inv_ref[8 * g:8 * g + 8, :] = jnp.where(row + 8 * g == lane, 1.0, 0.0).astype(jnp.float32)
    rd, ri = d_ref[:8, :], inv_ref[:8, :]
    c = [lane_bcast(rd, k) for k in range(8)]
    for s in range(n):
        follow = s + 1 < n
        if follow:
            rn, vn = d_ref[8 * s + 8:8 * s + 16, :], inv_ref[8 * s + 8:8 * s + 16, :]
            ca = [lane_bcast(rn, 8 * s + k) for k in range(8)]
            cb = [lane_bcast(rn, 8 * s + 8 + k) for k in range(8)]
        u = {}
        scale, ud, ui = [], [], []
        for j in range(8):
            rs = lax.rsqrt(sub_bcast(c[j], j))
            scale.append(rs)
            lj = jnp.where(row > j, c[j], 0.0) * rs
            for k in range(j + 1, 8):
                u[j, k] = sub_bcast(c[k], j) * rs
                c[k] = c[k] - lj * u[j, k]
            ud.append(sub_bcast(rd, j) * rs)
            ui.append(sub_bcast(ri, j) * rs)
            rd = rd - lj * ud[j]
            ri = ri - lj * ui[j]
            if follow:
                ln = ca[j] * rs
                for k in range(j + 1, 8):
                    ca[k] = ca[k] - ln * u[j, k]
                for k in range(8):
                    cb[k] = cb[k] - ln * sub_bcast(ln, k)
                rn = rn - ln * ud[j]
                vn = vn - ln * ui[j]
        out = ui[7]
        for j in range(7):
            out = jnp.where(row == j, ui[j], out)
        inv_ref[8 * s:8 * s + 8, :] = out
        for g in range(s + 2, n):
            rg = d_ref[8 * g:8 * g + 8, :]
            vg = inv_ref[8 * g:8 * g + 8, :]
            cg = [lane_bcast(rg, 8 * s + k) for k in range(8)]
            for j in range(8):
                lg = cg[j] * scale[j]
                for k in range(j + 1, 8):
                    cg[k] = cg[k] - lg * u[j, k]
                rg = rg - lg * ud[j]
                vg = vg - lg * ui[j]
            d_ref[8 * g:8 * g + 8, :] = rg
            inv_ref[8 * g:8 * g + 8, :] = vg
        if follow:
            c, rd, ri = cb, rn, vn


def scratch_of(nz, nc, cols, rows, wide):
    rank, half, chips = wide * nz, nz // 2, nc // 2
    thin, quarter, hi = wide // 2, nz // 4, rank // 2
    tall = (rank // nc) * (rank // 128) // nz
    win = window_rows(cols, nz)
    vm = pltpu.VMEM
    return dict(
        mom=vm((cols, rows), F32), grad=vm((cols, rows), BF16), blow=vm((cols, rows), BF16),
        held=vm((nz, 2, thin, cols), BF16),
        parts=vm((half, 2, chips, 8, 128), F32), mate=vm((half, chips, 8, 128), F32), came=vm((half, nc, 8, 128), F32),
        shares=vm((half, 2, chips, 8, 128), F32), w=vm((rank, rows), F32),
        gpart=vm((nz, tall, 128), F32), gcame=vm((nz, tall, 128), F32), grow=vm((nz, tall, 128), F32),
        gall=vm((2, chips, nz, tall, 128), F32),
        a=vm((rank, 2 * rank), F32), d=vm((NB, NB), F32), inv=vm((NB, NB), F32),
        y=vm((2, cols, hi), F32),
        leaf_came=vm((2, quarter, 2, win, hi), F32), stem=vm((2, quarter, 2, win, hi), F32),
        stem_came=vm((2, quarter, 2, win, hi), F32), own=vm((2, win, hi), F32),
        right=vm((nz, 2, win * (hi // 128), 128), BF16), r32=vm((cols, rank), F32),
        plow=vm((rank, rows), BF16), pt=vm((rows, rank), F32),
        sz=vm((nz, rank // 128, 128), F32), sx=vm((nc, rank // 128, 128), F32),
        q_ss=DMA((2, quarter, 2, 2)), q_rs=DMA((nz, 2)),
        b_ss=DMA((half,)), b_rs=DMA((half,)), c_ss=DMA((half,)), c_rs=DMA((half,)), a_ss=DMA((half,)), a_rs=DMA((half,)), d_ss=DMA((half,)), d_rs=DMA((half,)),
        z_ss=DMA, z_rs=DMA, y_ss=DMA, y_rs=DMA, g_ss=DMA, g_rs=DMA, e_ss=DMA, e_rs=DMA,
        l_ss=DMA((2, quarter, 2)), l_rs=DMA((2, quarter, 2)), r_ss=DMA((2, quarter, 2)), r_rs=DMA((2, quarter, 2)),
        p_ss=DMA((2, quarter, 2, 2)), p_rs=DMA((nz, 2)),
        n_ss=DMA, n_rs=DMA, m_ss=DMA, m_rs=DMA, i_s=DMA((4,)),
    )


def window_rows(cols, nz):
    return -(-(cols // nz) // 8) * 8


def window_start(i, cols, nz):
    return pl.multiple_of(lax.div(i * (cols // nz), 8) * 8, 8)


def split3(x):
    one = x.astype(BF16)
    rest = x - one.astype(F32)
    two = rest.astype(BF16)
    return one, two, (rest - two.astype(F32)).astype(BF16)


def kernel(nz, nc, mom_hbm, grad_hbm, q_hbm, m_out, p_out, q_out, s):
    z, c = lax.axis_index("row"), lax.axis_index("col")
    chip, core = lax.div(c, 2), lax.rem(c, 2)
    partner = chip * 2 + 1 - core
    chips, half = nc // 2, nz // 2
    wide = q_hbm.shape[0]
    thin = wide // 2
    cols, rows = s.blow.shape
    rank = wide * nz
    hi = rank // 2
    lanes = rows // 128

    def others(count):
        return pl.ds(0, count - 1)

    copies = [
        pltpu.make_async_copy(q_hbm.at[pl.ds(thin * chunk, thin)], s.held.at[0, chunk], s.i_s.at[chunk])
        for chunk in (0, 1)
    ]
    loads = [pltpu.make_async_copy(grad_hbm, s.grad, s.i_s.at[2]), pltpu.make_async_copy(mom_hbm, s.mom, s.i_s.at[3])]
    for copy in copies:
        copy.start()
    met = greet(z, c, nz, nc)
    for copy in loads:
        copy.start()
    for copy in copies:
        copy.wait()
    met()

    ring = Ring(s.held, s.q_ss, s.q_rs, z, nz)
    sides = [(t, (nz - t) % nz if t else half) for t in range(half)]
    late = (half - 1, 0)
    groups = [(2 * r - 1, 2 * r) for r in range(1, ring.rounds)] + [late]

    def multiply(*pairs):
        slots = [slot for p in pairs for slot in sides[p]]
        ring.slots_arrived(*slots)
        lhs = jnp.concatenate([s.held[slot].reshape(wide, -1) for slot in slots], axis=0)
        prod = jnp.dot(lhs, s.blow[...], preferred_element_type=F32)
        for i, p in enumerate(pairs):
            pass_on(p, prod[2 * wide * i:2 * wide * (i + 1)])
        for p in pairs:
            merge(p)

    def pass_on(p, prod):
        for side in (0, 1):
            for piece in range(chips):
                i, l = piece // lanes, piece % lanes
                s.parts[p, side, piece] = prod[side * wide + 8 * i:side * wide + 8 * i + 8, 128 * l:128 * l + 128]
        send(s.parts.at[p, 1 - core], s.mate.at[p], s.b_ss.at[p], s.b_rs.at[p], col=partner)

    def merge(p):
        drain(s.mate.at[p], s.b_rs.at[p])
        s.parts[p, core] = s.parts[p, core] + s.mate[p]
        s.came[p, chip] = s.parts[p, core, chip]

        @pl.loop(1, chips)
        def _(j):
            other = lax.rem(chip + j, chips)
            send(s.parts.at[p, core, other], s.came.at[p, chip], s.c_ss.at[p], s.c_rs.at[p], col=other * 2 + core)

    def add_up(p):
        drain(s.came.at[p, others(chips)], s.c_rs.at[p])
        s.shares[p, core, chip] = s.came[p, pl.ds(0, chips)].sum(axis=0)
        mine = s.shares.at[p, core, chip]
        if p in late:
            @pl.loop(1, nc)
            def _(j):
                send(mine, mine, s.a_ss.at[p], s.a_rs.at[p], col=lax.rem(c + j, nc))
        else:
            @pl.loop(1, chips)
            def _(j):
                send(mine, mine, s.a_ss.at[p], s.a_rs.at[p], col=lax.rem(chip + j, chips) * 2 + core)

    def cross(p):
        drain(s.shares.at[p, core, others(chips)], s.a_rs.at[p])
        view = s.shares.at[p, core]
        send(view, view, s.d_ss.at[p], s.d_rs.at[p], col=partner)

    ring.round(0)
    for copy in loads:
        copy.wait()
    s.blow[...] = (s.mom[...] + s.grad[...].astype(F32)).astype(BF16)
    for i in range(len(groups)):
        if i + 1 < ring.rounds:
            ring.round(i + 1)
        multiply(*groups[i])
        if i >= 2:
            for p in groups[i - 2]:
                add_up(p)
    for p in groups[-2]:
        add_up(p)
    for p in groups[0]:
        cross(p)
    for p in late:
        add_up(p)
    for group in groups[1:-1]:
        for p in group:
            cross(p)
    for p in range(half):
        if p in late:
            drain(s.came.at[p, others(nc)], s.a_rs.at[p])
        else:
            drain(s.shares.at[p, core], s.d_rs.at[p])
    for p in range(half):
        for side in (0, 1):
            at = lax.rem(z + nz - sides[p][side], nz) * wide
            for piece in range(chips):
                i, l = piece // lanes, piece % lanes
                s.w[pl.ds(pl.multiple_of(at + 8 * i, 8), 8), 128 * l:128 * l + 128] = s.shares[p, side, piece]

    share = rank // nc
    mine = s.w[pl.ds(pl.multiple_of(c * share, share), share), :]
    prod = lax.dot_general(mine, s.w[...], NT, precision=HI, preferred_element_type=F32)
    glanes = rank // 128
    tall = share * glanes // nz
    for piece in range(nz):
        i, l = piece // glanes, piece % glanes
        s.gpart[piece] = prod[tall * i:tall * (i + 1), 128 * l:128 * l + 128]
    s.gcame[z] = s.gpart[z]

    @pl.loop(1, nz)
    def _(j):
        to = lax.rem(z + j, nz)
        send(s.gpart.at[to], s.gcame.at[z], s.z_ss, s.z_rs, row=to)

    pieces = split3(s.w[...])
    for chunk in (0, 1):
        s.y[chunk] = sum(
            lax.dot_general(s.blow[...], piece[hi * chunk:hi * (chunk + 1)], NT, preferred_element_type=F32)
            for piece in reversed(pieces)
        )

    drain(s.gcame.at[others(nz)], s.z_rs)
    s.grow[z] = s.gcame[...].sum(axis=0)

    @pl.loop(1, nz)
    def _(j):
        send(s.grow.at[z], s.grow.at[z], s.y_ss, s.y_rs, row=lax.rem(z + j, nz))

    win = window_rows(cols, nz)
    to = [[lax.rem(z + step, nz) for step in (nz - hops, hops)] for hops in (1, 2)]

    def share_of(i, chunk):
        return s.y.at[chunk, pl.ds(window_start(i, cols, nz), win), :]

    def far_one(way, far):
        return lax.rem(z + (far if way else nz - far), nz)

    def inbound(came, sems, way, k, chunk):
        drain(came.at[way, k, chunk], sems.at[way, k, chunk])
        return came[way, k, chunk]

    def sum_round(far):
        k = far // 2
        for chunk in (0, 1):
            for way in (0, 1):
                if far == half and chunk != way:
                    continue
                value = share_of(far_one(way, far), chunk)[...]
                if far < half:
                    value = value + inbound(s.leaf_came, s.l_rs, way, k, chunk)
                if far < half - 2 or (far < half and chunk == way):
                    value = value + inbound(s.stem_came, s.r_rs, way, k, chunk)
                s.stem[way, k - 1, chunk] = value
                send(s.stem.at[way, k - 1, chunk], s.stem_came.at[way, k - 1, chunk],
                     s.r_ss.at[way, k - 1, chunk], s.r_rs.at[way, k - 1, chunk], row=to[1][way])
        for chunk in (0, 1):
            for way in (0, 1):
                send(share_of(far_one(way, far - 1), chunk), s.leaf_came.at[way, k - 1, chunk],
                     s.l_ss.at[way, k - 1, chunk], s.l_rs.at[way, k - 1, chunk], row=to[0][way])

    sum_round(half)
    drain(s.grow.at[others(nz)], s.y_rs)
    s.gall[core, chip] = s.grow[...]

    @pl.loop(1, chips)
    def _(j):
        mine = s.gall.at[core, chip]
        send(mine, mine, s.g_ss, s.g_rs, col=lax.rem(chip + j, chips) * 2 + core)

    row = lax.broadcasted_iota(jnp.int32, (NB, rank), 0)
    lane = lax.broadcasted_iota(jnp.int32, (NB, rank), 1)
    for b in range(rank // NB):
        s.a[NB * b:NB * (b + 1), rank:] = jnp.where(row + NB * b == lane, 1.0, 0.0).astype(F32)
    sum_round(half - 2)
    drain(s.gall.at[core, others(chips)], s.g_rs)
    across = send(s.gall.at[core], s.gall.at[core], s.e_ss, s.e_rs, col=partner)
    across.wait()
    for other in range(nc):
        for piece in range(nz):
            i, l = piece // glanes, piece % glanes
            top = other * share + tall * i
            s.a[top:top + tall, 128 * l:128 * l + 128] = s.gall[other % 2, other // 2, piece]

    sum_round(half - 4)

    blocks = rank // NB

    def step(b, carry):
        at = pl.multiple_of(b * NB, NB)
        s.d[...] = s.a[pl.ds(at, NB), pl.ds(at, NB)]
        diag_inverse(s.d, s.inv)
        for bb in range(blocks):
            @pl.when(b == bb)
            def _():
                low, top = bb * NB, (bb + 1) * NB
                prod = jnp.dot(s.inv[...], s.a[low:top, top:rank + top], precision=HI, preferred_element_type=F32)
                s.a[low:top, rank:rank + top] = prod[:, rank - top:]
                if bb < blocks - 1:
                    ut = prod[:, :rank - top].T
                    s.a[top:rank, top:rank + top] = s.a[top:rank, top:rank + top] - jnp.dot(
                        ut, prod, precision=HI, preferred_element_type=F32)
                if bb == 1:
                    for far in range(half - 6, 0, -2):
                        sum_round(far)
        return carry

    lax.fori_loop(0, blocks, step, 0)

    for chunk in (0, 1):
        value = share_of(z, chunk)[...]
        for way in (0, 1):
            value = value + inbound(s.leaf_came, s.l_rs, way, 0, chunk) + inbound(s.stem_came, s.r_rs, way, 0, chunk)
        s.own[chunk] = value
    right = sum(
        lax.dot_general(s.own[chunk], s.a[:, rank + hi * chunk:rank + hi * (chunk + 1)], NT,
                        precision=HI, preferred_element_type=F32)
        for chunk in (0, 1)
    )
    before = lax.rem(z + nz - 1, nz)
    seen = jnp.where(z == 0, 0, window_start(before, cols, nz) + win - window_start(z, cols, nz))
    fresh = lax.broadcasted_iota(jnp.int32, right.shape, 0) >= seen
    squares = jnp.sum(jnp.where(fresh, right * right, 0.0), axis=0, keepdims=True)
    for l in range(glanes):
        s.sz[z, l:l + 1, :] = squares[:, 128 * l:128 * l + 128]

    @pl.loop(1, nz)
    def _(j):
        send(s.sz.at[z], s.sz.at[z], s.n_ss, s.n_rs, row=lax.rem(z + j, nz))

    for chunk in (0, 1):
        strips = [right[:, hi * chunk + 128 * l:hi * chunk + 128 * (l + 1)] for l in range(hi // 128)]
        s.right[0, chunk] = jnp.concatenate(strips, axis=0).astype(BF16)
    gather = Ring(s.right, s.p_ss, s.p_rs, z, nz)
    gather.round(0)

    p = jnp.dot(s.a[:, rank:], s.w[...], precision=HI, preferred_element_type=F32)
    s.plow[...] = p.astype(BF16)
    s.pt[...] = p.T
    out = p_out.shape[0]
    p_out[...] = s.pt[pl.ds(pl.multiple_of(c * out, out), out), :]

    for r in range(1, gather.rounds - 1):
        gather.round(r)
    drain(s.sz.at[others(nz)], s.n_rs)
    s.sx[c] = s.sz[...].sum(axis=0)

    @pl.loop(1, nc)
    def _(j):
        send(s.sx.at[c], s.sx.at[c], s.m_ss, s.m_rs, col=lax.rem(c + j, nc))

    gather.round(gather.rounds - 1)
    drain(s.sx.at[others(nc)], s.m_rs)
    total = s.sx[...].sum(axis=0)
    total = jnp.concatenate([total[l:l + 1, :] for l in range(glanes)], axis=1)
    pick = lax.broadcasted_iota(jnp.int32, (wide, rank), 1) == lax.broadcasted_iota(jnp.int32, (wide, rank), 0) + z * wide
    norms = jnp.sqrt(jnp.sum(jnp.where(pick, total, 0.0), axis=1, keepdims=True) + 1e-06)
    gather.slots_arrived(*range(nz))
    for slot in range(nz):
        at = window_start(lax.rem(z + nz - slot, nz), cols, nz)
        for chunk in (0, 1):
            strips = s.right[slot, chunk].astype(F32)
            for l in range(hi // 128):
                left = hi * chunk + 128 * l
                s.r32[pl.ds(at, win), left:left + 128] = strips[win * l:win * (l + 1)]
    low = s.r32[...].astype(BF16)
    update = jnp.dot(low, s.plow[...], preferred_element_type=F32)
    m_out[...] = (0.1 * update).astype(BF16)
    q_out[...] = lax.dot_general(jnp.where(pick, 1.0, 0.0).astype(BF16), low, NT, preferred_element_type=F32) / norms

    ring.finish()
    gather.finish()
    for p in range(half):
        drain(s.mate.at[p], s.b_ss.at[p])
        drain(s.came.at[p, others(chips)], s.c_ss.at[p])
        if p in late:
            drain(s.came.at[p, others(nc)], s.a_ss.at[p])
        else:
            drain(s.shares.at[p, core, others(chips)], s.a_ss.at[p])
            drain(s.shares.at[p, core], s.d_ss.at[p])
    drain(s.gcame.at[others(nz)], s.z_ss)
    drain(s.grow.at[others(nz)], s.y_ss)
    drain(s.gall.at[core, others(chips)], s.g_ss)
    drain(s.sz.at[others(nz)], s.n_ss)
    drain(s.sx.at[others(nc)], s.m_ss)
    for way in (0, 1):
        for k in range(half // 2):
            for chunk in (0, 1):
                drain(s.leaf_came.at[way, k, chunk], s.l_ss.at[way, k, chunk])
                if k < half // 2 - 1 or chunk == way:
                    drain(s.stem_came.at[way, k, chunk], s.r_ss.at[way, k, chunk])


def run(mom, grad, q, nz, nc):
    cols, rows = mom.shape
    wide = q.shape[0]
    rank = wide * nz
    scratch = scratch_of(nz, nc, cols, rows, wide)
    names = list(scratch)
    whole = pl.BlockSpec(memory_space=pltpu.VMEM)
    return pl.pallas_call(
        lambda *refs: kernel(nz, nc, *refs[:6], SimpleNamespace(**dict(zip(names, refs[6:])))),
        out_shape=(
            jax.ShapeDtypeStruct((cols, rows), BF16),
            jax.ShapeDtypeStruct((rows // nc, rank), F32),
            jax.ShapeDtypeStruct((wide, cols), F32),
        ),
        in_specs=[pl.BlockSpec(memory_space=pltpu.HBM)] * 3,
        out_specs=(whole,) * 3,
        scratch_shapes=list(scratch.values()),
        compiler_params=pltpu.CompilerParams(collective_id=0, has_side_effects=True, vmem_limit_bytes=67043328),
        name="dion",
    )(mom, grad, q)


def solution(mesh):
    nz, nc = mesh.shape["row"], mesh.shape["col"]

    def body(momentum, gradient, q_basis):
        change, p_out, q_next = run(momentum.T, gradient.T, q_basis.T, nz, nc)
        mom_next = (momentum + gradient.astype(F32)) - change.T.astype(F32)
        return mom_next, p_out, q_next.T

    placed = (P("row", "col"), P("row", "col"), P("col", "row"))
    return jax.shard_map(
        body, mesh=mesh, in_specs=placed, out_specs=(P("row", "col"), P(("row", "col"), None), P("col", "row")),
        check_vma=False,
    )
```

```python
from types import SimpleNamespace

import jax
import jax.numpy as jnp
from jax import lax
from jax.experimental import pallas as pl
from jax.experimental.pallas import tpu as pltpu
from jax.sharding import PartitionSpec as P

HI = lax.Precision.HIGHEST
MESH = pl.DeviceIdType.MESH
F32, BF16 = jnp.float32, jnp.bfloat16
NB = 128
DMA = pltpu.SemaphoreType.DMA
NT = (((1,), (1,)), ((), ()))
TN = (((0,), (0,)), ((), ()))


def send(src, dst, send_sem, recv_sem, **where):
    copy = pltpu.make_async_remote_copy(
        src_ref=src, dst_ref=dst, send_sem=send_sem, recv_sem=recv_sem, device_id=where, device_id_type=MESH
    )
    copy.start()
    return copy


def drain(view, sem):
    pltpu.make_async_copy(view, view, sem).wait()


def greet(z, c, nz, nc):
    barrier = pltpu.get_barrier_semaphore()
    near = (1, 2, nz - 2, nz - 1)
    for step in near:
        pl.semaphore_signal(barrier, inc=1, device_id={"row": lax.rem(z + step, nz)}, device_id_type=MESH)

    @pl.loop(1, nc)
    def _(j):
        pl.semaphore_signal(barrier, inc=1, device_id={"col": lax.rem(c + j, nc)}, device_id_type=MESH)

    def met():
        pl.semaphore_wait(barrier, len(near) + nc - 1)

    return met


class Ring:
    def __init__(self, held, send_sems, recv_sems, z, nz):
        self.held, self.ss, self.rs = held, send_sems, recv_sems
        self.nz, self.half = nz, nz // 2
        self.rounds = self.half // 2
        self.to = [[lax.rem(z + step, nz) for step in (hops, nz - hops)] for hops in (1, 2)]
        self.sent, self.got = [], set()

    def arrived(self, slot, chunk):
        if slot != 0 and (slot, chunk) not in self.got:
            self.got.add((slot, chunk))
            drain(self.held.at[slot, chunk], self.rs.at[slot, chunk])

    def slots_arrived(self, *slots):
        for slot in slots:
            for chunk in (0, 1):
                self.arrived(slot % self.nz, chunk)

    def round(self, r):
        for hops in (2, 1):
            for chunk in (0, 1):
                for way in (0, 1):
                    src, dst = 2 * r, 2 * r + hops
                    if dst == self.half and chunk != way:
                        continue
                    if way:
                        src, dst = (self.nz - src) % self.nz, self.nz - dst
                    self.arrived(src, chunk)
                    self.sent.append(send(
                        self.held.at[src, chunk], self.held.at[dst, chunk],
                        self.ss.at[way, r, hops - 1, chunk], self.rs.at[dst, chunk], row=self.to[hops - 1][way]))

    def finish(self):
        for copy in self.sent:
            copy.wait_send()


def sub_bcast(x, j):
    return jnp.broadcast_to(x[j:j + 1, :], x.shape)


def lane_bcast(x, j):
    return jnp.broadcast_to(x[:, j:j + 1], x.shape)


def diag_inverse(d_ref, inv_ref):
    n = NB // 8
    row = lax.broadcasted_iota(jnp.int32, (8, NB), 0)
    lane = lax.broadcasted_iota(jnp.int32, (8, NB), 1)
    for g in range(n):
        inv_ref[8 * g:8 * g + 8, :] = jnp.where(row + 8 * g == lane, 1.0, 0.0).astype(jnp.float32)
    rd, ri = d_ref[:8, :], inv_ref[:8, :]
    c = [lane_bcast(rd, k) for k in range(8)]
    for s in range(n):
        follow = s + 1 < n
        if follow:
            rn, vn = d_ref[8 * s + 8:8 * s + 16, :], inv_ref[8 * s + 8:8 * s + 16, :]
            ca = [lane_bcast(rn, 8 * s + k) for k in range(8)]
            cb = [lane_bcast(rn, 8 * s + 8 + k) for k in range(8)]
        u = {}
        scale, ud, ui = [], [], []
        for j in range(8):
            rs = lax.rsqrt(sub_bcast(c[j], j))
            scale.append(rs)
            lj = jnp.where(row > j, c[j], 0.0) * rs
            for k in range(j + 1, 8):
                u[j, k] = sub_bcast(c[k], j) * rs
                c[k] = c[k] - lj * u[j, k]
            ud.append(sub_bcast(rd, j) * rs)
            ui.append(sub_bcast(ri, j) * rs)
            rd = rd - lj * ud[j]
            ri = ri - lj * ui[j]
            if follow:
                ln = ca[j] * rs
                for k in range(j + 1, 8):
                    ca[k] = ca[k] - ln * u[j, k]
                for k in range(8):
                    cb[k] = cb[k] - ln * sub_bcast(ln, k)
                rn = rn - ln * ud[j]
                vn = vn - ln * ui[j]
        out = ui[7]
        for j in range(7):
            out = jnp.where(row == j, ui[j], out)
        inv_ref[8 * s:8 * s + 8, :] = out
        for g in range(s + 2, n):
            rg = d_ref[8 * g:8 * g + 8, :]
            vg = inv_ref[8 * g:8 * g + 8, :]
            cg = [lane_bcast(rg, 8 * s + k) for k in range(8)]
            for j in range(8):
                lg = cg[j] * scale[j]
                for k in range(j + 1, 8):
                    cg[k] = cg[k] - lg * u[j, k]
                rg = rg - lg * ud[j]
                vg = vg - lg * ui[j]
            d_ref[8 * g:8 * g + 8, :] = rg
            inv_ref[8 * g:8 * g + 8, :] = vg
        if follow:
            c, rd, ri = cb, rn, vn


def scratch_of(nz, nc, cols, rows, wide):
    rank, half, chips = wide * nz, nz // 2, nc // 2
    thin, quarter, hi = wide // 2, nz // 4, rank // 2
    tall = (rank // nc) * (rank // 128) // nz
    win = window_rows(cols, nz)
    vm = pltpu.VMEM
    return dict(
        mom=vm((cols, rows), F32), grad=vm((cols, rows), BF16), blow=vm((cols, rows), BF16),
        held=vm((nz, 2, thin, cols), BF16),
        parts=vm((half, 2, chips, 8, 128), F32), mate=vm((half, chips, 8, 128), F32), came=vm((half, nc, 8, 128), F32),
        shares=vm((half, 2, chips, 8, 128), F32), w=vm((rank, rows), F32),
        gpart=vm((nz, tall, 128), F32), gcame=vm((nz, tall, 128), F32), grow=vm((nz, tall, 128), F32),
        gall=vm((2, chips, nz, tall, 128), F32),
        a=vm((rank, 2 * rank), F32), d=vm((NB, NB), F32), inv=vm((NB, NB), F32),
        y=vm((2, cols, hi), F32),
        leaf_came=vm((2, quarter, 2, win, hi), F32), stem=vm((2, quarter, 2, win, hi), F32),
        stem_came=vm((2, quarter, 2, win, hi), F32), own=vm((2, win, hi), F32),
        right=vm((nz, 2, win * (hi // 128), 128), BF16), r32=vm((cols, rank), F32),
        plow=vm((rank, rows), BF16), pt=vm((rows, rank), F32),
        sz=vm((nz, rank // 128, 128), F32), sx=vm((nc, rank // 128, 128), F32),
        q_ss=DMA((2, quarter, 2, 2)), q_rs=DMA((nz, 2)),
        b_ss=DMA((half,)), b_rs=DMA((half,)), c_ss=DMA((half,)), c_rs=DMA((half,)), a_ss=DMA((half,)), a_rs=DMA((half,)), d_ss=DMA((half,)), d_rs=DMA((half,)),
        z_ss=DMA, z_rs=DMA, y_ss=DMA, y_rs=DMA, g_ss=DMA, g_rs=DMA, e_ss=DMA, e_rs=DMA,
        l_ss=DMA((2, quarter, 2)), l_rs=DMA((2, quarter, 2)), r_ss=DMA((2, quarter, 2)), r_rs=DMA((2, quarter, 2)),
        p_ss=DMA((2, quarter, 2, 2)), p_rs=DMA((nz, 2)),
        n_ss=DMA, n_rs=DMA, m_ss=DMA, m_rs=DMA, i_s=DMA((4,)),
    )


def window_rows(cols, nz):
    return -(-(cols // nz) // 8) * 8


def window_start(i, cols, nz):
    return pl.multiple_of(lax.div(i * (cols // nz), 8) * 8, 8)


def split3(x):
    one = x.astype(BF16)
    rest = x - one.astype(F32)
    two = rest.astype(BF16)
    return one, two, (rest - two.astype(F32)).astype(BF16)


def kernel(nz, nc, mom_hbm, grad_hbm, q_hbm, m_out, p_out, q_out, s):
    z, c = lax.axis_index("row"), lax.axis_index("col")
    chip, core = lax.div(c, 2), lax.rem(c, 2)
    partner = chip * 2 + 1 - core
    chips, half = nc // 2, nz // 2
    wide = q_hbm.shape[0]
    thin = wide // 2
    cols, rows = s.blow.shape
    rank = wide * nz
    hi = rank // 2
    lanes = rows // 128

    def others(count):
        return pl.ds(0, count - 1)

    copies = [
        pltpu.make_async_copy(q_hbm.at[pl.ds(thin * chunk, thin)], s.held.at[0, chunk], s.i_s.at[chunk])
        for chunk in (0, 1)
    ]
    loads = [pltpu.make_async_copy(grad_hbm, s.grad, s.i_s.at[2]), pltpu.make_async_copy(mom_hbm, s.mom, s.i_s.at[3])]
    for copy in copies:
        copy.start()
    met = greet(z, c, nz, nc)
    for copy in loads:
        copy.start()
    for copy in copies:
        copy.wait()
    met()

    ring = Ring(s.held, s.q_ss, s.q_rs, z, nz)
    sides = [(t, (nz - t) % nz if t else half) for t in range(half)]
    late = (half - 1, 0)
    groups = [(2 * r - 1, 2 * r) for r in range(1, ring.rounds)] + [late]

    def multiply(*pairs):
        slots = [slot for p in pairs for slot in sides[p]]
        ring.slots_arrived(*slots)
        lhs = jnp.concatenate([s.held[slot].reshape(wide, -1) for slot in slots], axis=0)
        prod = jnp.dot(lhs, s.blow[...], preferred_element_type=F32)
        for i, p in enumerate(pairs):
            pass_on(p, prod[2 * wide * i:2 * wide * (i + 1)])
        for p in pairs:
            merge(p)

    def pass_on(p, prod):
        for side in (0, 1):
            for piece in range(chips):
                i, l = piece // lanes, piece % lanes
                s.parts[p, side, piece] = prod[side * wide + 8 * i:side * wide + 8 * i + 8, 128 * l:128 * l + 128]
        send(s.parts.at[p, 1 - core], s.mate.at[p], s.b_ss.at[p], s.b_rs.at[p], col=partner)

    def merge(p):
        drain(s.mate.at[p], s.b_rs.at[p])
        s.parts[p, core] = s.parts[p, core] + s.mate[p]
        s.came[p, chip] = s.parts[p, core, chip]

        @pl.loop(1, chips)
        def _(j):
            other = lax.rem(chip + j, chips)
            send(s.parts.at[p, core, other], s.came.at[p, chip], s.c_ss.at[p], s.c_rs.at[p], col=other * 2 + core)

    def add_up(p):
        drain(s.came.at[p, others(chips)], s.c_rs.at[p])
        s.shares[p, core, chip] = s.came[p, pl.ds(0, chips)].sum(axis=0)
        mine = s.shares.at[p, core, chip]
        if p in late:
            @pl.loop(1, nc)
            def _(j):
                send(mine, mine, s.a_ss.at[p], s.a_rs.at[p], col=lax.rem(c + j, nc))
        else:
            @pl.loop(1, chips)
            def _(j):
                send(mine, mine, s.a_ss.at[p], s.a_rs.at[p], col=lax.rem(chip + j, chips) * 2 + core)

    def cross(p):
        drain(s.shares.at[p, core, others(chips)], s.a_rs.at[p])
        view = s.shares.at[p, core]
        send(view, view, s.d_ss.at[p], s.d_rs.at[p], col=partner)

    ring.round(0)
    for copy in loads:
        copy.wait()
    s.blow[...] = (s.mom[...] + s.grad[...].astype(F32)).astype(BF16)
    for i in range(len(groups)):
        if i + 1 < ring.rounds:
            ring.round(i + 1)
        multiply(*groups[i])
        if i >= 2:
            for p in groups[i - 2]:
                add_up(p)
    for p in groups[-2]:
        add_up(p)
    for p in groups[0]:
        cross(p)
    for p in late:
        add_up(p)
    for group in groups[1:-1]:
        for p in group:
            cross(p)
    for p in range(half):
        if p in late:
            drain(s.came.at[p, others(nc)], s.a_rs.at[p])
        else:
            drain(s.shares.at[p, core], s.d_rs.at[p])
    for p in range(half):
        for side in (0, 1):
            at = lax.rem(z + nz - sides[p][side], nz) * wide
            for piece in range(chips):
                i, l = piece // lanes, piece % lanes
                s.w[pl.ds(pl.multiple_of(at + 8 * i, 8), 8), 128 * l:128 * l + 128] = s.shares[p, side, piece]

    share = rank // nc
    mine = s.w[pl.ds(pl.multiple_of(c * share, share), share), :]
    prod = lax.dot_general(mine, s.w[...], NT, precision=HI, preferred_element_type=F32)
    glanes = rank // 128
    tall = share * glanes // nz
    for piece in range(nz):
        i, l = piece // glanes, piece % glanes
        s.gpart[piece] = prod[tall * i:tall * (i + 1), 128 * l:128 * l + 128]
    s.gcame[z] = s.gpart[z]

    @pl.loop(1, nz)
    def _(j):
        to = lax.rem(z + j, nz)
        send(s.gpart.at[to], s.gcame.at[z], s.z_ss, s.z_rs, row=to)

    pieces = split3(s.w[...])
    for chunk in (0, 1):
        s.y[chunk] = sum(
            lax.dot_general(s.blow[...], piece[hi * chunk:hi * (chunk + 1)], NT, preferred_element_type=F32)
            for piece in reversed(pieces)
        )

    drain(s.gcame.at[others(nz)], s.z_rs)
    s.grow[z] = s.gcame[...].sum(axis=0)

    @pl.loop(1, nz)
    def _(j):
        send(s.grow.at[z], s.grow.at[z], s.y_ss, s.y_rs, row=lax.rem(z + j, nz))

    win = window_rows(cols, nz)
    to = [[lax.rem(z + step, nz) for step in (nz - hops, hops)] for hops in (1, 2)]

    def share_of(i, chunk):
        return s.y.at[chunk, pl.ds(window_start(i, cols, nz), win), :]

    def far_one(way, far):
        return lax.rem(z + (far if way else nz - far), nz)

    def inbound(came, sems, way, k, chunk):
        drain(came.at[way, k, chunk], sems.at[way, k, chunk])
        return came[way, k, chunk]

    def sum_round(far):
        k = far // 2
        for chunk in (0, 1):
            for way in (0, 1):
                if far == half and chunk != way:
                    continue
                value = share_of(far_one(way, far), chunk)[...]
                if far < half:
                    value = value + inbound(s.leaf_came, s.l_rs, way, k, chunk)
                if far < half - 2 or (far < half and chunk == way):
                    value = value + inbound(s.stem_came, s.r_rs, way, k, chunk)
                s.stem[way, k - 1, chunk] = value
                send(s.stem.at[way, k - 1, chunk], s.stem_came.at[way, k - 1, chunk],
                     s.r_ss.at[way, k - 1, chunk], s.r_rs.at[way, k - 1, chunk], row=to[1][way])
        for chunk in (0, 1):
            for way in (0, 1):
                send(share_of(far_one(way, far - 1), chunk), s.leaf_came.at[way, k - 1, chunk],
                     s.l_ss.at[way, k - 1, chunk], s.l_rs.at[way, k - 1, chunk], row=to[0][way])

    sum_round(half)
    drain(s.grow.at[others(nz)], s.y_rs)
    s.gall[core, chip] = s.grow[...]

    @pl.loop(1, chips)
    def _(j):
        mine = s.gall.at[core, chip]
        send(mine, mine, s.g_ss, s.g_rs, col=lax.rem(chip + j, chips) * 2 + core)

    row = lax.broadcasted_iota(jnp.int32, (NB, rank), 0)
    lane = lax.broadcasted_iota(jnp.int32, (NB, rank), 1)
    for b in range(rank // NB):
        s.a[NB * b:NB * (b + 1), rank:] = jnp.where(row + NB * b == lane, 1.0, 0.0).astype(F32)
    sum_round(half - 2)
    drain(s.gall.at[core, others(chips)], s.g_rs)
    across = send(s.gall.at[core], s.gall.at[core], s.e_ss, s.e_rs, col=partner)
    across.wait()
    for other in range(nc):
        for piece in range(nz):
            i, l = piece // glanes, piece % glanes
            top = other * share + tall * i
            s.a[top:top + tall, 128 * l:128 * l + 128] = s.gall[other % 2, other // 2, piece]

    sum_round(half - 4)

    blocks = rank // NB

    def step(b, carry):
        at = pl.multiple_of(b * NB, NB)
        s.d[...] = s.a[pl.ds(at, NB), pl.ds(at, NB)]
        diag_inverse(s.d, s.inv)
        for bb in range(blocks):
            @pl.when(b == bb)
            def _():
                low, top = bb * NB, (bb + 1) * NB
                prod = jnp.dot(s.inv[...], s.a[low:top, top:rank + top], precision=HI, preferred_element_type=F32)
                s.a[low:top, rank:rank + top] = prod[:, rank - top:]
                if bb < blocks - 1:
                    ut = prod[:, :rank - top].T
                    s.a[top:rank, top:rank + top] = s.a[top:rank, top:rank + top] - jnp.dot(
                        ut, prod, precision=HI, preferred_element_type=F32)
                if bb == 1:
                    for far in range(half - 6, 0, -2):
                        sum_round(far)
        return carry

    lax.fori_loop(0, blocks, step, 0)

    for chunk in (0, 1):
        value = share_of(z, chunk)[...]
        for way in (0, 1):
            value = value + inbound(s.leaf_came, s.l_rs, way, 0, chunk) + inbound(s.stem_came, s.r_rs, way, 0, chunk)
        s.own[chunk] = value
    right = sum(
        lax.dot_general(s.own[chunk], s.a[:, rank + hi * chunk:rank + hi * (chunk + 1)], NT,
                        precision=HI, preferred_element_type=F32)
        for chunk in (0, 1)
    )
    before = lax.rem(z + nz - 1, nz)
    seen = jnp.where(z == 0, 0, window_start(before, cols, nz) + win - window_start(z, cols, nz))
    fresh = lax.broadcasted_iota(jnp.int32, right.shape, 0) >= seen
    squares = jnp.sum(jnp.where(fresh, right * right, 0.0), axis=0, keepdims=True)
    for l in range(glanes):
        s.sz[z, l:l + 1, :] = squares[:, 128 * l:128 * l + 128]

    @pl.loop(1, nz)
    def _(j):
        send(s.sz.at[z], s.sz.at[z], s.n_ss, s.n_rs, row=lax.rem(z + j, nz))

    for chunk in (0, 1):
        strips = [right[:, hi * chunk + 128 * l:hi * chunk + 128 * (l + 1)] for l in range(hi // 128)]
        s.right[0, chunk] = jnp.concatenate(strips, axis=0).astype(BF16)
    gather = Ring(s.right, s.p_ss, s.p_rs, z, nz)
    gather.round(0)

    p = jnp.dot(s.a[:, rank:], s.w[...], precision=HI, preferred_element_type=F32)
    s.plow[...] = p.astype(BF16)
    s.pt[...] = p.T
    out = p_out.shape[0]
    p_out[...] = s.pt[pl.ds(pl.multiple_of(c * out, out), out), :]

    for r in range(1, gather.rounds - 1):
        gather.round(r)
    drain(s.sz.at[others(nz)], s.n_rs)
    s.sx[c] = s.sz[...].sum(axis=0)

    @pl.loop(1, nc)
    def _(j):
        send(s.sx.at[c], s.sx.at[c], s.m_ss, s.m_rs, col=lax.rem(c + j, nc))

    gather.round(gather.rounds - 1)
    drain(s.sx.at[others(nc)], s.m_rs)
    total = s.sx[...].sum(axis=0)
    total = jnp.concatenate([total[l:l + 1, :] for l in range(glanes)], axis=1)
    pick = lax.broadcasted_iota(jnp.int32, (wide, rank), 1) == lax.broadcasted_iota(jnp.int32, (wide, rank), 0) + z * wide
    norms = jnp.sqrt(jnp.sum(jnp.where(pick, total, 0.0), axis=1, keepdims=True) + 1e-06)
    gather.slots_arrived(*range(nz))
    for slot in range(nz):
        at = window_start(lax.rem(z + nz - slot, nz), cols, nz)
        for chunk in (0, 1):
            strips = s.right[slot, chunk].astype(F32)
            for l in range(hi // 128):
                left = hi * chunk + 128 * l
                s.r32[pl.ds(at, win), left:left + 128] = strips[win * l:win * (l + 1)]
    low = s.r32[...].astype(BF16)
    update = jnp.dot(low, s.plow[...], preferred_element_type=F32)
    m_out[...] = (s.mom[...] + s.grad[...].astype(F32)) - 0.1 * update
    q_out[...] = lax.dot_general(jnp.where(pick, 1.0, 0.0).astype(BF16), low, NT, preferred_element_type=F32) / norms

    ring.finish()
    gather.finish()
    for p in range(half):
        drain(s.mate.at[p], s.b_ss.at[p])
        drain(s.came.at[p, others(chips)], s.c_ss.at[p])
        if p in late:
            drain(s.came.at[p, others(nc)], s.a_ss.at[p])
        else:
            drain(s.shares.at[p, core, others(chips)], s.a_ss.at[p])
            drain(s.shares.at[p, core], s.d_ss.at[p])
    drain(s.gcame.at[others(nz)], s.z_ss)
    drain(s.grow.at[others(nz)], s.y_ss)
    drain(s.gall.at[core, others(chips)], s.g_ss)
    drain(s.sz.at[others(nz)], s.n_ss)
    drain(s.sx.at[others(nc)], s.m_ss)
    for way in (0, 1):
        for k in range(half // 2):
            for chunk in (0, 1):
                drain(s.leaf_came.at[way, k, chunk], s.l_ss.at[way, k, chunk])
                if k < half // 2 - 1 or chunk == way:
                    drain(s.stem_came.at[way, k, chunk], s.r_ss.at[way, k, chunk])


def run(mom, grad, q, nz, nc):
    cols, rows = mom.shape
    wide = q.shape[0]
    rank = wide * nz
    scratch = scratch_of(nz, nc, cols, rows, wide)
    names = list(scratch)
    whole = pl.BlockSpec(memory_space=pltpu.VMEM)
    return pl.pallas_call(
        lambda *refs: kernel(nz, nc, *refs[:6], SimpleNamespace(**dict(zip(names, refs[6:])))),
        out_shape=(
            jax.ShapeDtypeStruct((cols, rows), F32),
            jax.ShapeDtypeStruct((rows // nc, rank), F32),
            jax.ShapeDtypeStruct((wide, cols), F32),
        ),
        in_specs=[pl.BlockSpec(memory_space=pltpu.HBM)] * 3,
        out_specs=(whole,) * 3,
        scratch_shapes=list(scratch.values()),
        compiler_params=pltpu.CompilerParams(collective_id=0, has_side_effects=True, vmem_limit_bytes=40 * 1024 * 1024),
        name="dion",
    )(*(pltpu.with_memory_space_constraint(x, pltpu.HBM) for x in (mom, grad, q)))


def solution(mesh):
    nz, nc = mesh.shape["row"], mesh.shape["col"]

    def body(momentum, gradient, q_basis):
        mom_next, p_out, q_next = run(momentum.T, gradient.T, q_basis.T, nz, nc)
        return mom_next.T, p_out, q_next.T

    placed = (P("row", "col"), P("row", "col"), P("col", "row"))
    return jax.shard_map(
        body, mesh=mesh, in_specs=placed, out_specs=(P("row", "col"), P(("row", "col"), None), P("col", "row")),
        check_vma=False,
    )
```
